256 devices in a mesh: row: 16 (over z, y_hi), ma: 16 (over y_lo, x, core).
Axes of the slice: x: 4, y: 4 (y_hi: 2, y_lo: 2; y = y_hi * 2 + y_lo), z: 8, core: 2. Of those that a mesh axis runs over, the one named last changes fastest.
Arguments:
- thermal_state: float32 [128, 768, 2048], P('row', None, 'ma'), may hold values from -6 to 6
- sphere_node_annulus: int32 [128, 768], P('row'), may hold values from 0 to 1022, as said below
- sphere_node_offset: float32 [128, 768], P('row'), may hold values from 0 to 1
- integration_share: float32 [128, 768], P('row'), may hold values from 0.02 to 0.2
- annulus_holder_row: int32 [1024], replicated, may hold values from 0 to 15, never falling along the last dimension, each value on 1 to 128 neighbouring positions
- rotating_flow_potential: float32 [2048, 2048], P('row', 'ma'), may hold values from -6 to 6
Outputs:
- thermal_state_later: float32 [128, 768, 2048], P('row', None, 'ma')
- flow_potential_later: float32 [2048, 2048], P('row', 'ma')
The draws below stay inside these ranges and needn't reach their ends.
Inputs may be any that keep to these rules, and one draw needn't show every extreme that they name: `sphere_node_annulus`: lower cell of each point; the next cell exists. `annulus_holder_row`: never falling along cells; each owner holds 1 to 128 cells and some owner exactly 128.
All inputs are finite; a program needn't handle non-finite values.
Results may differ from the reference program's by a relative error of at most 0.0003.
Values sent between devices are 32-bit elements; how exact they have to be, the bound alone decides.
A program may use at most 64 MiB of HBM per device.

```python
import math
import jax
import jax.numpy as jnp
import numpy as np
from jax import lax

NS = 1024
LONGITUDE_NODES = 2048
MERIDIAN_NODES = 768
SPHERE_LEVELS = 128
S_MOST = 128
OWNER_SLOTS = 2048
N_ROW = 16


def draw_sphere_node_annulus(key, part):
    centre_distance = jnp.arange(SPHERE_LEVELS, dtype=jnp.int32)[:, None]
    colatitude = jnp.arange(MERIDIAN_NODES, dtype=jnp.int32)[None, :]
    inner_radius = 7 * SPHERE_LEVELS // 13
    sine_level = 4 * (colatitude + 1) * (MERIDIAN_NODES - colatitude) * 1024 // ((MERIDIAN_NODES + 1) * (MERIDIAN_NODES + 1))
    column_base = (inner_radius + centre_distance) * sine_level * (NS - 2) // ((inner_radius + SPHERE_LEVELS) * 1024)
    jitter = jax.random.randint(key, (SPHERE_LEVELS, MERIDIAN_NODES), -1, 2, dtype=jnp.int32)
    return jnp.clip(column_base + jitter, 0, NS - 2).astype(jnp.int32)


def levels(key, shape, pieces, least, high):
    level = 1.0
    for dim, shards_of in pieces:
        draws = jax.random.uniform(jax.random.fold_in(jax.random.fold_in(key, 6), dim), (shards_of,), jnp.float32, least / len(pieces), high / len(pieces))
        level = level * jnp.repeat(jnp.exp(draws), shape[dim] // shards_of).reshape((-1,) + (1,) * (len(shape) - 1 - dim))
    return level


def length_profile(number_of, total, reach, lean):
    portions = [(1 << 20) // math.isqrt(grade ** lean) + 1 for grade in range(2, number_of + 1)]
    surplus, counts = total - reach - (number_of - 1), [1] * (number_of - 1)
    while surplus > 0:
        candidates = [i for i in range(number_of - 1) if counts[i] < reach]
        whole, budget = sum([portions[i] for i in candidates]), surplus
        for i in candidates:
            extra = min(reach - counts[i], max(1, budget * portions[i] // whole), surplus)
            counts[i] = counts[i] + extra
            surplus = surplus - extra
    return np.array([reach] + counts)


def uneven_parts(stream_key, amount, total, bound, skew):
    if amount == 2:
        one = jax.random.randint(stream_key, (), max(1, total - bound), min(bound, total - 1) + 1)
        return jnp.stack([one, total - one])
    sizes = jnp.asarray(length_profile(amount, total, bound, skew), jnp.int32)
    pairs = (amount - 1) // 2
    donor, taker = sizes[1:1 + 2 * pairs:2], sizes[2:2 + 2 * pairs:2]
    margin = jnp.minimum(donor - 1, bound - taker)
    passed = jax.random.randint(jax.random.fold_in(stream_key, 1), (pairs,), 0, 1 << 20) % (margin + 1)
    sizes = sizes.at[1:1 + 2 * pairs:2].set(donor - passed).at[2:2 + 2 * pairs:2].set(taker + passed)
    return sizes[jax.random.permutation(jax.random.fold_in(stream_key, 2), amount)]


def normal_values(rng, shape, spread, reach, shards=(), held_as=jnp.bfloat16):
    result = jax.random.normal(rng, shape, jnp.float32) * spread
    if len(shards) > 0:
        result = levels(rng, shape, shards, -0.22, 0.18) * result
    return jnp.clip(result, min=-reach, max=reach).astype(held_as)


def setup_inputs(seed: int = 0) -> dict:
    seeds = jax.random.split(jax.random.key(seed), 7)
    thermal_state = normal_values(seeds[0], (SPHERE_LEVELS, MERIDIAN_NODES, LONGITUDE_NODES), 1.0, 6.0, ((0, 16), (2, 16)), jnp.float32)
    sphere_node_annulus = draw_sphere_node_annulus(jax.random.fold_in(seeds[6], 71), 0)
    sphere_node_offset = jnp.clip(1.0 * jax.random.uniform(seeds[2], (SPHERE_LEVELS, MERIDIAN_NODES), jnp.float32) ** levels(seeds[2], (SPHERE_LEVELS, MERIDIAN_NODES), ((0, 16),), -0.2, 0.2), 0.0, 1.0)
    integration_share = jnp.clip(jnp.exp(math.log(0.2) - 2.3025851 * jax.random.uniform(seeds[3], (SPHERE_LEVELS, MERIDIAN_NODES), jnp.float32) ** levels(seeds[3], (SPHERE_LEVELS, MERIDIAN_NODES), ((0, 16),), -0.2, 0.2)), 0.02, 0.2)
    annulus_holder_row = jnp.searchsorted(jnp.cumsum(uneven_parts(seeds[4], N_ROW, NS, S_MOST, 2)), jnp.arange(NS), side="right").astype(jnp.int32)
    rotating_flow_potential = normal_values(seeds[5], (OWNER_SLOTS, LONGITUDE_NODES), 1.0, 6.0, ((0, 16), (1, 16)), jnp.float32)
    return dict(thermal_state=thermal_state, sphere_node_annulus=sphere_node_annulus, sphere_node_offset=sphere_node_offset, integration_share=integration_share, annulus_holder_row=annulus_holder_row, rotating_flow_potential=rotating_flow_potential)


stream_step = 0.5
thermal_advance = 0.25


def reference(thermal_state, sphere_node_annulus, sphere_node_offset, integration_share, annulus_holder_row, rotating_flow_potential):
    cells = jnp.arange(NS, dtype=jnp.int32)
    before = jnp.sum((annulus_holder_row[None, :] < annulus_holder_row[:, None]).astype(jnp.int32), axis=1)
    slot_of_cell = (annulus_holder_row * S_MOST + cells - before).astype(jnp.int32)
    geo = 1.0 / (0.25 + (cells.astype(jnp.float32) + 0.5) / NS)
    below_share = integration_share * (1.0 - sphere_node_offset)
    above_share = integration_share * sphere_node_offset

    def accumulate(total, items):
        plane, lower, low_w, high_w = items
        total = total + jax.ops.segment_sum(low_w[:, None] * plane, lower, num_segments=NS)
        total = total + jax.ops.segment_sum(high_w[:, None] * plane, lower + 1, num_segments=NS)
        return total, None

    zint, _ = lax.scan(accumulate, jnp.zeros((NS, LONGITUDE_NODES), jnp.float32),
                       (thermal_state, sphere_node_annulus, below_share, above_share))
    forcing = -geo[:, None] * ((jnp.roll(zint, -1, 1) - jnp.roll(zint, 1, 1)) * 0.5)
    stream_cell = rotating_flow_potential[slot_of_cell] + stream_step * forcing
    flow_potential_later = rotating_flow_potential.at[slot_of_cell].set(stream_cell)
    velocity = geo[:, None] * ((jnp.roll(stream_cell, -1, 1) - jnp.roll(stream_cell, 1, 1)) * 0.5)
    angle = math.pi * (jnp.arange(MERIDIAN_NODES, dtype=jnp.float32) + 0.5) / MERIDIAN_NODES
    sin_theta_term = jnp.sin(angle)[:, None]
    cos_theta_term = jnp.cos(angle)[:, None]

    def march_forward(centre_distance):
        present_entry = thermal_state[centre_distance]
        preceding_entry = jnp.where(centre_distance > 0, thermal_state[jnp.maximum(centre_distance - 1, 0)], 0.0)
        successor_entry = jnp.where(centre_distance < SPHERE_LEVELS - 1, thermal_state[jnp.minimum(centre_distance + 1, SPHERE_LEVELS - 1)], 0.0)
        distance_from_centre = (successor_entry - preceding_entry) * 0.5
        wrapped_heat_grid = jnp.pad(present_entry, ((1, 1), (0, 0)))
        theta_from_north = (wrapped_heat_grid[2:] - wrapped_heat_grid[:-2]) * 0.5
        lower = sphere_node_annulus[centre_distance]
        fraction = sphere_node_offset[centre_distance][:, None]
        shifted_heat = (1.0 - fraction) * velocity[lower] + fraction * velocity[lower + 1]
        return present_entry - thermal_advance * shifted_heat * (sin_theta_term * distance_from_centre + cos_theta_term * theta_from_north)

    thermal_state_later = lax.map(march_forward, jnp.arange(SPHERE_LEVELS, dtype=jnp.int32))
    return thermal_state_later, flow_potential_later
```

```python
import functools
import math

import jax
import jax.numpy as jnp
import numpy as np
from jax import lax
from jax.experimental import pallas as pl
from jax.experimental.pallas import tpu as pltpu
from jax.sharding import PartitionSpec as P

MESH = pl.DeviceIdType.MESH
F32 = jnp.float32
BF16 = jnp.bfloat16
N_ROW = 16
N_MA = 16
NT = (((1,), (1,)), ((), ()))


def two_parts(x):
    hi = x.astype(BF16)
    return hi, (x - hi.astype(F32)).astype(BF16)


def one_hot(rows, first, index):
    at = lax.broadcasted_iota(jnp.int32, (rows, index.shape[1]), 0)
    return jnp.where(at == index - first, 1.0, 0.0).astype(BF16)


def geo_row(cells):
    c = lax.broadcasted_iota(jnp.int32, (1, cells), 1).astype(F32)
    return 1.0 / (0.25 + (c + 0.5) / cells)


def own_slots(holder, me, slots):
    cells = holder.shape[1]
    start = jnp.sum((holder < me).astype(F32), axis=1, keepdims=True).astype(jnp.int32)
    c = lax.broadcasted_iota(jnp.int32, (1, cells), 1)
    return one_hot(slots, 0, jnp.where(holder == me, c - start, -1))


def integrate_kernel(t_hbm, low_ref, off_ref, share_ref, holder_ref, stream_ref, sp_ref, edge_ref, tv, twt, lower_sum, upper_sum, sems):
    levels, nodes, width = tv.shape
    cells = holder_ref.shape[1]
    tile = 256
    copies = [pltpu.make_async_copy(t_hbm.at[r], tv.at[r], sems.at[r]) for r in range(levels)]
    for copy in copies:
        copy.start()
    me = lax.axis_index("row")
    geo = geo_row(cells)
    spots = own_slots(holder_ref[...], me, stream_ref.shape[0])
    stream = jnp.concatenate(two_parts(stream_ref[...].T), axis=0)
    placed = jnp.dot(stream, spots, preferred_element_type=F32)
    stream = placed[:width] + placed[width:]
    for r in range(levels):
        copies[r].wait()
        share = share_ref[r : r + 1, :]
        offset = off_ref[r : r + 1, :]
        heat = tv[r].T
        for k, weight in enumerate((share * (1.0 - offset), share * offset)):
            hi, lo = two_parts(heat * weight)
            twt[r, 2 * k * width : (2 * k + 1) * width, :] = hi
            twt[r, (2 * k + 1) * width : (2 * k + 2) * width, :] = lo

    def step(n, carry):
        total = jnp.zeros((4 * width, tile), F32)
        for r in range(levels):
            marks = one_hot(tile, n * tile, low_ref[r : r + 1, :])
            total = total + lax.dot_general(twt[r], marks, NT, preferred_element_type=F32)
        at = pl.ds(pl.multiple_of(n * tile, tile), tile)
        lower_sum[:, at] = total[:width] + total[width : 2 * width]
        upper_sum[:, at] = total[2 * width : 3 * width] + total[3 * width :]
        return carry

    lax.fori_loop(0, cells // tile, step, 0)
    zint = 0.25 * geo * (lower_sum[...] + pltpu.roll(upper_sum[...], 1, axis=1))
    zero = jnp.zeros((1, cells), F32)
    ahead = jnp.concatenate([zint[1:], zero], axis=0)
    behind = jnp.concatenate([zero, zint[:-1]], axis=0)
    partial = stream - (ahead - behind)
    sp_ref[...] = partial
    edge_ref[0] = jnp.concatenate([zint[:1], partial[:1]], axis=0)
    edge_ref[1] = jnp.concatenate([zint[-1:], partial[-1:]], axis=0)


def exchange_kernel(t_hbm, sp_ref, edge_ref, sall_ref, eall_ref, under_ref, over_ref, rim, ends, rim_send, rs_buf, rim_buf, own, rim_own, rs_send, rs_recv, e_send, e_recv, ag_send, ag_recv, ea_send, ea_recv, ma_send, ma_recv, h_send, h_recv):
    me = lax.axis_index("row")
    ma = lax.axis_index("ma")
    right, left = lax.rem(ma + 1, N_MA), lax.rem(ma + N_MA - 1, N_MA)
    cells = sp_ref.shape[2]
    levels, nodes = t_hbm.shape[:2]
    parts = h_send.shape[1]
    piece = nodes // parts

    barrier = pltpu.get_barrier_semaphore()
    for d in range(1, N_ROW):
        pl.semaphore_signal(barrier, inc=1, device_id={"row": lax.rem(me + d, N_ROW)}, device_id_type=MESH)
    for side in (left, right):
        pl.semaphore_signal(barrier, inc=1, device_id={"ma": side}, device_id_type=MESH)
    pl.semaphore_wait(barrier, N_ROW + 1)

    def to_row(src, dst, send, recv, peer):
        return pltpu.make_async_remote_copy(src_ref=src, dst_ref=dst, send_sem=send, recv_sem=recv, device_id={"row": peer}, device_id_type=MESH)

    def halo(side, k):
        peer = jnp.maximum(me - 1, 0) if side == 0 else jnp.minimum(me + 1, N_ROW - 1)
        at = pl.ds(k * piece, piece)
        return to_row(
            t_hbm.at[0 if side == 0 else levels - 1, at],
            (over_ref if side == 0 else under_ref).at[at],
            h_send.at[side, k],
            h_recv.at[side, k],
            peer,
        )

    def halo_start(first, last):
        for side, there in ((0, me > 0), (1, me < N_ROW - 1)):

            @pl.when(there)
            def _(side=side):
                for k in range(first, last):
                    halo(side, k).start()

    rims = [
        pltpu.make_async_remote_copy(src_ref=edge_ref.at[k], dst_ref=rim.at[k], send_sem=ma_send.at[k], recv_sem=ma_recv.at[k], device_id={"ma": side}, device_id_type=MESH)
        for k, side in enumerate((left, right))
    ]
    for copy in rims:
        copy.start()
    for d in range(1, N_ROW):
        peer = lax.rem(me + d, N_ROW)

        @pl.when(jnp.logical_and(peer > 0, peer < N_ROW - 1))
        def _(d=d, peer=peer):
            to_row(sp_ref.at[peer], rs_buf.at[d], rs_send.at[d], rs_recv.at[d], peer).start()

    for copy in rims:
        copy.wait()
    ends[0] = sp_ref[0]
    ends[1] = sp_ref[N_ROW - 1]
    ends[0, 0:1] = sp_ref[0, 0:1] + rim[1, 0:1]
    ends[1, 7:8] = sp_ref[N_ROW - 1, 7:8] - rim[0, 0:1]
    outer = (rim[1, 1:2] - edge_ref[0, 0:1], rim[0, 1:2] + edge_ref[1, 0:1])
    for p in range(N_ROW):
        at = p % 8
        rim_send[p] = outer[p // 8][:, at * 128 : (at + 1) * 128]
    for k, p in enumerate((0, N_ROW - 1)):

        @pl.when(me != p)
        def _(k=k, p=p):
            d = lax.rem(p - me + N_ROW, N_ROW)
            to_row(ends.at[k], rs_buf.at[d], rs_send.at[d], rs_recv.at[d], p).start()

    e_out = []
    for d in range(1, N_ROW):
        peer = lax.rem(me + d, N_ROW)
        e_out.append(to_row(rim_send.at[peer], rim_buf.at[d], e_send.at[d], e_recv.at[d], peer))
        e_out[-1].start()
    half = parts // 2
    halo_start(0, half)

    def rs_copy(d):
        return to_row(sp_ref.at[0], rs_buf.at[d], rs_send.at[d], rs_recv.at[d], lax.rem(me + d, N_ROW))

    total = jnp.where(me == 0, ends[0], jnp.where(me == N_ROW - 1, ends[1], sp_ref[me]))
    rim_total = rim_send[me]
    for d in range(1, N_ROW):
        rs_copy(d).wait_recv()
        total = total + rs_buf[d]
    for d in range(1, N_ROW):
        e_out[d - 1].wait_recv()
        rim_total = rim_total + rim_buf[d]
    own[...] = total
    rim_own[...] = rim_total
    sall_ref[me] = total
    eall_ref[me] = rim_total
    ag = []
    for d in range(1, N_ROW):
        peer = lax.rem(me + d, N_ROW)
        ag.append(to_row(own, sall_ref.at[me], ag_send.at[d], ag_recv.at[d], peer))
        ag.append(to_row(rim_own, eall_ref.at[me], ea_send.at[d], ea_recv.at[d], peer))
    for copy in ag:
        copy.start()
    halo_start(half, parts)
    for d in range(1, N_ROW):
        rs_copy(d).wait_send()
        e_out[d - 1].wait_send()
    for copy in ag:
        copy.wait()
    for side, there, comes in ((0, me > 0, me < N_ROW - 1), (1, me < N_ROW - 1, me > 0)):

        @pl.when(there)
        def _(side=side):
            for k in range(parts):
                halo(side, k).wait_send()

        @pl.when(comes)
        def _(side=side):
            for k in range(parts):
                halo(side, k).wait_recv()


def advance_kernel(t_hbm, under_hbm, over_hbm, low_ref, off_ref, holder_ref, stream_ref, sin_ref, cos_ref, sall_ref, eall_ref, out_hbm, flow_ref, tp, vel, out, sems, out_sems):
    levels, nodes, width = out.shape
    cells = holder_ref.shape[1]
    tile = 256
    me = lax.axis_index("row")
    body = pl.ds(8, nodes)
    sources = [under_hbm] + [t_hbm.at[r] for r in range(levels)] + [over_hbm]
    copies = [pltpu.make_async_copy(src, tp.at[r, body], sems.at[r]) for r, src in enumerate(sources)]
    for copy in copies:
        copy.start()
    for r in range(levels):
        tp[r + 1, 0:8] = jnp.zeros((8, width), F32)
        tp[r + 1, nodes + 8 : nodes + 16] = jnp.zeros((8, width), F32)
    stream = sall_ref[...].reshape(width, cells)
    spots = own_slots(holder_ref[...], me, stream_ref.shape[0])
    parts = jnp.concatenate(two_parts(stream), axis=0)
    held = lax.dot_general(parts, spots, NT, preferred_element_type=F32)
    held = (held[:width] + held[width:]).T
    count = jnp.sum((holder_ref[...] == me).astype(F32), axis=1, keepdims=True).astype(jnp.int32)
    slot = lax.broadcasted_iota(jnp.int32, held.shape, 0)
    flow_ref[...] = jnp.where(slot < count, held, stream_ref[...])

    first = jnp.concatenate([eall_ref[p] for p in range(8)], axis=1)
    last = jnp.concatenate([eall_ref[p] for p in range(8, 16)], axis=1)
    ahead = jnp.concatenate([stream[1:], last], axis=0)
    behind = jnp.concatenate([first, stream[:-1]], axis=0)
    velocity = (0.5 * geo_row(cells)) * (ahead - behind)
    change = pltpu.roll(velocity, cells - 1, axis=1) - velocity
    for k, x in enumerate(two_parts(velocity) + two_parts(change)):
        vel[k * width : (k + 1) * width, :] = x
    for copy in copies:
        copy.wait()

    @pl.when(me == 0)
    def _():
        tp[0, 8 : nodes + 8] = jnp.zeros((nodes, width), F32)

    @pl.when(me == N_ROW - 1)
    def _():
        tp[levels + 1, 8 : nodes + 8] = jnp.zeros((nodes, width), F32)

    def step(r, carry):
        for k in range(nodes // tile):
            at = slice(k * tile, (k + 1) * tile)
            marks = one_hot(cells, 0, low_ref[pl.ds(r, 1), at])
            both = jnp.dot(vel[...], marks, preferred_element_type=F32)
            drift = both[:width] + both[width : 2 * width]
            drift = drift + off_ref[pl.ds(r, 1), at] * (both[2 * width : 3 * width] + both[3 * width :])
            drift = drift.T
            lo, hi = 8 + k * tile, 8 + (k + 1) * tile
            radial = tp[r + 2, lo:hi] - tp[r, lo:hi]
            polar = tp[r + 1, lo + 1 : hi + 1] - tp[r + 1, lo - 1 : hi - 1]
            out[r, at] = tp[r + 1, lo:hi] - drift * (sin_ref[at] * radial + cos_ref[at] * polar)
        pltpu.make_async_copy(out.at[r], out_hbm.at[r], out_sems.at[r]).start()
        return carry

    lax.fori_loop(0, levels, step, 0)
    for r in range(levels):
        pltpu.make_async_copy(out.at[r], out_hbm.at[r], out_sems.at[r]).wait()


VMEM = pl.BlockSpec(memory_space=pltpu.VMEM)
ANY = pl.BlockSpec(memory_space=pl.ANY)
DMA = pltpu.SemaphoreType.DMA


def per_device(heat, lower, offset, share, holder, stream):
    levels, nodes, width = heat.shape
    cells = holder.shape[0]
    slots = stream.shape[0]
    holder = holder.reshape(1, cells)
    angle = math.pi * (np.arange(nodes, dtype=np.float32) + np.float32(0.5)) / nodes
    sines = jnp.asarray(np.repeat((0.125 * np.sin(angle)).astype(np.float32)[:, None], width, axis=1))
    cosines = jnp.asarray(np.repeat((0.125 * np.cos(angle)).astype(np.float32)[:, None], width, axis=1))
    params = functools.partial(pltpu.CompilerParams, vmem_limit_bytes=48 << 20)

    partial, edges = pl.pallas_call(
        integrate_kernel,
        out_shape=(jax.ShapeDtypeStruct((width, cells), F32), jax.ShapeDtypeStruct((2, 2, cells), F32)),
        in_specs=[ANY] + [VMEM] * 5,
        out_specs=(VMEM, VMEM),
        scratch_shapes=[
            pltpu.VMEM((levels, nodes, width), F32),
            pltpu.VMEM((levels, 4 * width, nodes), BF16),
            pltpu.VMEM((width, cells), F32),
            pltpu.VMEM((width, cells), F32),
            DMA((levels,)),
        ],
        compiler_params=params(),
        name="integrate",
    )(heat, lower, offset, share, holder, stream)

    rows = width // N_ROW
    parts = 6
    sem = lambda: DMA((N_ROW,))
    sall, eall, under, over = pl.pallas_call(
        exchange_kernel,
        out_shape=(
            jax.ShapeDtypeStruct((N_ROW, rows, cells), F32),
            jax.ShapeDtypeStruct((N_ROW, 1, 128), F32),
            jax.ShapeDtypeStruct((nodes, width), F32),
            jax.ShapeDtypeStruct((nodes, width), F32),
        ),
        in_specs=[ANY, VMEM, VMEM],
        out_specs=(VMEM, VMEM, ANY, ANY),
        scratch_shapes=[
            pltpu.VMEM((2, 2, cells), F32),
            pltpu.VMEM((2, rows, cells), F32),
            pltpu.VMEM((N_ROW, 1, 128), F32),
            pltpu.VMEM((N_ROW, rows, cells), F32),
            pltpu.VMEM((N_ROW, 1, 128), F32),
            pltpu.VMEM((rows, cells), F32),
            pltpu.VMEM((1, 128), F32),
            sem(), sem(), sem(), sem(), sem(), sem(), sem(), sem(),
            DMA((2,)), DMA((2,)), DMA((2, parts)), DMA((2, parts)),
        ],
        compiler_params=params(collective_id=0, has_side_effects=True),
        name="exchange",
    )(heat, partial.reshape(N_ROW, rows, cells), edges)

    return pl.pallas_call(
        advance_kernel,
        out_shape=(jax.ShapeDtypeStruct(heat.shape, F32), jax.ShapeDtypeStruct((slots, width), F32)),
        in_specs=[ANY] * 3 + [VMEM] * 8,
        out_specs=(ANY, VMEM),
        scratch_shapes=[
            pltpu.VMEM((levels + 2, nodes + 16, width), F32),
            pltpu.VMEM((4 * width, cells), BF16),
            pltpu.VMEM((levels, nodes, width), F32),
            DMA((levels + 2,)),
            DMA((levels,)),
        ],
        compiler_params=params(),
        name="advance",
    )(heat, under, over, lower, offset, holder, stream, sines, cosines, sall, eall)


def solution(mesh):
    return jax.shard_map(
        per_device,
        mesh=mesh,
        in_specs=(P("row", None, "ma"), P("row", None), P("row", None), P("row", None), P(), P("row", "ma")),
        out_specs=(P("row", None, "ma"), P("row", "ma")),
        check_vma=False,
    )
```

```python
import functools
import math

import jax
import jax.numpy as jnp
import numpy as np
from jax import lax
from jax.experimental import pallas as pl
from jax.experimental.pallas import tpu as pltpu
from jax.sharding import PartitionSpec as P

MESH = pl.DeviceIdType.MESH
F32 = jnp.float32
BF16 = jnp.bfloat16
N_ROW = 16
N_MA = 16
NT = (((1,), (1,)), ((), ()))


def two_parts(x):
    hi = x.astype(BF16)
    return hi, (x - hi.astype(F32)).astype(BF16)


def one_hot(rows, first, index):
    at = lax.broadcasted_iota(jnp.int32, (rows, index.shape[1]), 0)
    return jnp.where(at == index - first, 1.0, 0.0).astype(BF16)


def geo_row(cells, first, count):
    c = (first + lax.broadcasted_iota(jnp.int32, (1, count), 1)).astype(F32)
    return 1.0 / (0.25 + (c + 0.5) / cells)


def own_slots(holder, me, slots):
    cells = holder.shape[1]
    start = jnp.sum((holder < me).astype(F32), axis=1, keepdims=True).astype(jnp.int32)
    c = lax.broadcasted_iota(jnp.int32, (1, cells), 1)
    return one_hot(slots, 0, jnp.where(holder == me, c - start, -1))


def fused_kernel(
    t_hbm, low_hbm, off_hbm, share_hbm, holder_hbm, stream_hbm,
    tv, pvt, vel_last, sall,
    low, off, share, holder, stream_in, stream, twt, sp, edge, rim, ends, rim_send, rs_buf, rim_buf, own, rim_own, eall, carry_up, carry_vel, vel,
    t_sem, in_sem, rs_send, rs_recv, ag_send, ag_recv, e_send, e_recv, ea_send, ea_recv, ma_send, ma_recv, h_send, h_recv,
):
    levels, width, nodes = pvt.shape
    cells = holder.shape[1]
    stages, tile = sp.shape[0], sp.shape[3]
    me = lax.axis_index("row")
    ma = lax.axis_index("ma")
    right, left = lax.rem(ma + 1, N_MA), lax.rem(ma + N_MA - 1, N_MA)
    parts = h_send.shape[1]
    piece = nodes // parts

    small = [(holder_hbm, holder), (stream_hbm, stream_in), (share_hbm, share), (off_hbm, off), (low_hbm, low)]
    loads = [pltpu.make_async_copy(src, dst, in_sem.at[k]) for k, (src, dst) in enumerate(small)]
    heat_loads = [pltpu.make_async_copy(t_hbm.at[r], tv.at[r + 1], t_sem.at[r]) for r in range(levels)]
    for copy in loads + heat_loads:
        copy.start()
    barrier = pltpu.get_barrier_semaphore()
    for d in range(1, N_ROW):
        pl.semaphore_signal(barrier, inc=1, device_id={"row": lax.rem(me + d, N_ROW)}, device_id_type=MESH)
    for side in (left, right):
        pl.semaphore_signal(barrier, inc=1, device_id={"ma": side}, device_id_type=MESH)

    @pl.when(me == 0)
    def _():
        tv[0] = jnp.zeros((nodes, width), F32)

    @pl.when(me == N_ROW - 1)
    def _():
        tv[levels + 1] = jnp.zeros((nodes, width), F32)

    for copy in loads:
        copy.wait()
    spots = own_slots(holder[...], me, stream_in.shape[0])
    placed = jnp.dot(jnp.concatenate(two_parts(stream_in[...].T), axis=0), spots, preferred_element_type=F32)
    stream[...] = placed[:width] + placed[width:]
    for r in range(levels):
        heat_loads[r].wait()
        weights = share[r : r + 1, :]
        offset = off[r : r + 1, :]
        heat = tv[r + 1].T
        for k, weight in enumerate((weights * (1.0 - offset), weights * offset)):
            hi, lo = two_parts(heat * weight)
            twt[r, 2 * k * width : (2 * k + 1) * width, :] = hi
            twt[r, (2 * k + 1) * width : (2 * k + 2) * width, :] = lo

    pl.semaphore_wait(barrier, N_ROW + 1)

    def to_row(src, dst, send, recv, peer):
        return pltpu.make_async_remote_copy(src_ref=src, dst_ref=dst, send_sem=send, recv_sem=recv, device_id={"row": peer}, device_id_type=MESH)

    def halo(side, k):
        peer = jnp.maximum(me - 1, 0) if side == 0 else jnp.minimum(me + 1, N_ROW - 1)
        at = pl.ds(k * piece, piece)
        mine, theirs = (1, levels + 1) if side == 0 else (levels, 0)
        return to_row(tv.at[mine, at], tv.at[theirs, at], h_send.at[side, k], h_recv.at[side, k], peer)

    def halo_start(first, last):
        for side, there in ((0, me > 0), (1, me < N_ROW - 1)):

            @pl.when(there)
            def _(side=side):
                for k in range(first, last):
                    halo(side, k).start()

    def pieces(n):
        return (2 * n, 2 * n + 1, 8 + 2 * n, 8 + 2 * n + 1)

    def rim_copies(n):
        return [
            pltpu.make_async_remote_copy(src_ref=edge.at[n, k], dst_ref=rim.at[n, k], send_sem=ma_send.at[n, k], recv_sem=ma_recv.at[n, k], device_id={"ma": side}, device_id_type=MESH)
            for k, side in enumerate((left, right))
        ]

    def rs_copy(n, d, src):
        return to_row(src, rs_buf.at[n, d], rs_send.at[n, d], rs_recv.at[n, d], lax.rem(me + d, N_ROW))

    def ag_copy(n, d):
        return to_row(own.at[n], sall.at[n, me], ag_send.at[n, d], ag_recv.at[n, d], lax.rem(me + d, N_ROW))

    def e_copy(p, d):
        return to_row(rim_send.at[p], rim_buf.at[d], e_send.at[d], e_recv.at[d], p)

    def ea_copy(d):
        return to_row(rim_own, eall.at[me], ea_send.at[d], ea_recv.at[me], lax.rem(me + d, N_ROW))

    def sum_columns(n):
        total = jnp.zeros((4 * width, tile), F32)
        for r in range(levels):
            marks = one_hot(tile, n * tile, low[r : r + 1, :])
            total = total + lax.dot_general(twt[r], marks, NT, preferred_element_type=F32)
        lower = total[:width] + total[width : 2 * width]
        upper = pltpu.roll(total[2 * width : 3 * width] + total[3 * width :], 1, axis=1)
        lane = lax.broadcasted_iota(jnp.int32, (width, 128), 1)
        before = jnp.zeros((width, 128), F32) if n == 0 else carry_up[...]
        carry_up[...] = upper[:, :128]
        upper = jnp.concatenate([jnp.where(lane == 0, before, upper[:, :128]), upper[:, 128:]], axis=1)
        zint = (0.25 * geo_row(cells, n * tile, tile)) * (lower + upper)
        zero = jnp.zeros((1, tile), F32)
        ahead = jnp.concatenate([zint[1:], zero], axis=0)
        behind = jnp.concatenate([zero, zint[:-1]], axis=0)
        partial = stream[:, n * tile : (n + 1) * tile] - (ahead - behind)
        sp[n] = partial.reshape(N_ROW, width // N_ROW, tile)
        edge[n, 0] = jnp.concatenate([zint[:1], partial[:1]], axis=0)
        edge[n, 1] = jnp.concatenate([zint[-1:], partial[-1:]], axis=0)

    def send_inner(n):
        for copy in rim_copies(n):
            copy.start()
        for d in range(1, N_ROW):
            peer = lax.rem(me + d, N_ROW)

            @pl.when(jnp.logical_and(peer > 0, peer < N_ROW - 1))
            def _(d=d, peer=peer):
                rs_copy(n, d, sp.at[n, peer]).start()

    def send_outer(n):
        for copy in rim_copies(n):
            copy.wait()
        last = width // N_ROW - 1
        ends[n, 0] = sp[n, 0]
        ends[n, 1] = sp[n, N_ROW - 1]
        ends[n, 0, 0:1] = sp[n, 0, 0:1] + rim[n, 1, 0:1]
        ends[n, 1, last : last + 1] = sp[n, N_ROW - 1, last : last + 1] - rim[n, 0, 0:1]
        outer = (rim[n, 1, 1:2] - edge[n, 0, 0:1], rim[n, 0, 1:2] + edge[n, 1, 0:1])
        for i, p in enumerate(pieces(n)):
            rim_send[p] = outer[i // 2][:, (i % 2) * 128 : (i % 2 + 1) * 128]
        for k, p in enumerate((0, N_ROW - 1)):

            @pl.when(me != p)
            def _(k=k, p=p):
                rs_copy(n, lax.rem(p - me + N_ROW, N_ROW), ends.at[n, k]).start()

        for p in pieces(n):

            @pl.when(me != p)
            def _(p=p):
                e_copy(p, lax.rem(p - me + N_ROW, N_ROW)).start()

    def reduce_rows(n):
        total = jnp.where(me == 0, ends[n, 0], jnp.where(me == N_ROW - 1, ends[n, 1], sp[n, me]))
        for d in range(1, N_ROW):
            rs_copy(n, d, own.at[n]).wait_recv()
            total = total + rs_buf[n, d]
        own[n] = total
        sall[n, me] = total
        for d in range(1, N_ROW):
            ag_copy(n, d).start()

        @pl.when(lax.rem(me, 8) // 2 == n)
        def _():
            total = rim_send[me]
            for d in range(1, N_ROW):
                e_copy(0, d).wait_recv()
                total = total + rim_buf[d]
            rim_own[...] = total
            eall[me] = total
            for d in range(1, N_ROW):
                ea_copy(d).start()

    def velocity(n):
        for d in range(1, N_ROW):
            ag_copy(n, d).wait_recv()
        for p in pieces(n):

            @pl.when(me != p)
            def _(p=p):
                to_row(rim_own, eall.at[p], ea_send.at[0], ea_recv.at[p], p).wait_recv()

        field = sall[n].reshape(width, tile)
        first, last = (jnp.concatenate([eall[p], eall[p + 1]], axis=1) for p in (2 * n, 8 + 2 * n))
        ahead = jnp.concatenate([field[1:], last], axis=0)
        behind = jnp.concatenate([first, field[:-1]], axis=0)
        now = (0.5 * geo_row(cells, n * tile, tile)) * (ahead - behind)
        lane = lax.broadcasted_iota(jnp.int32, (width, 128), 1)
        down = pltpu.roll(now, 1, axis=1)
        before = jnp.zeros((width, 128), F32) if n == 0 else carry_vel[...]
        carry_vel[...] = down[:, :128]
        down = jnp.concatenate([jnp.where(lane == 0, before, down[:, :128]), down[:, 128:]], axis=1)
        into = vel_last if n == stages - 1 else vel
        for k, x in enumerate(two_parts(down) + two_parts(now - down)):
            into[k * width : (k + 1) * width, :] = x

    def interpolate(n):
        def step(r, carry):
            for k in range(nodes // 256):
                at = slice(k * 256, (k + 1) * 256)
                marks = one_hot(tile, n * tile - 1, low[pl.ds(r, 1), at])
                both = jnp.dot(vel[...], marks, preferred_element_type=F32)
                part = both[:width] + both[width : 2 * width]
                part = part + off[pl.ds(r, 1), at] * (both[2 * width : 3 * width] + both[3 * width :])
                pvt[r, :, at] = part if n == 0 else pvt[r, :, at] + part
            return carry

        lax.fori_loop(0, levels, step, 0)

    halo_start(0, 2)
    for n in range(stages):
        sum_columns(n)
        send_inner(n)
        if n > 0:
            send_outer(n - 1)
        halo_start(n + 2, n + 3)
    send_outer(stages - 1)
    for n in range(stages):
        reduce_rows(n)
        halo_start(n + 6, n + 7)
    halo_start(10, parts)
    for n in range(stages):
        velocity(n)
        if n < stages - 1:
            interpolate(n)
    for n in range(stages):
        for d in range(1, N_ROW):
            rs_copy(n, d, own.at[n]).wait_send()
            ag_copy(n, d).wait_send()
    for d in range(1, N_ROW):
        e_copy(0, d).wait_send()
        ea_copy(d).wait_send()
    for side, there, comes in ((0, me > 0, me < N_ROW - 1), (1, me < N_ROW - 1, me > 0)):

        @pl.when(there)
        def _(side=side):
            for k in range(parts):
                halo(side, k).wait_send()

        @pl.when(comes)
        def _(side=side):
            for k in range(parts):
                halo(side, k).wait_recv()


def advance_kernel(tv, pvt, vel, sall, low, off, holder, stream, sines, cosines, out_hbm, flow, out, out_sem):
    levels, nodes, width = out.shape
    cells = holder.shape[1]
    stages, tile = sall.shape[0], sall.shape[3]
    me = lax.axis_index("row")

    def step(r, carry):
        for k in range(nodes // 256):
            lo, hi = k * 256, (k + 1) * 256
            at = slice(lo, hi)
            marks = one_hot(tile, (stages - 1) * tile - 1, low[pl.ds(r, 1), at])
            both = jnp.dot(vel[...], marks, preferred_element_type=F32)
            drift = pvt[r, :, at] + both[:width] + both[width : 2 * width]
            drift = drift + off[pl.ds(r, 1), at] * (both[2 * width : 3 * width] + both[3 * width :])
            drift = drift.T
            zero = jnp.zeros((1, width), F32)
            south = jnp.concatenate([tv[r + 1, lo + 1 : hi], zero], axis=0) if hi == nodes else tv[r + 1, lo + 1 : hi + 1]
            north = jnp.concatenate([zero, tv[r + 1, lo : hi - 1]], axis=0) if lo == 0 else tv[r + 1, lo - 1 : hi - 1]
            radial = tv[r + 2, at] - tv[r, at]
            out[r, at] = tv[r + 1, at] - drift * (sines[at] * radial + cosines[at] * (south - north))
        pltpu.make_async_copy(out.at[r], out_hbm.at[r], out_sem.at[r]).start()
        return carry

    lax.fori_loop(0, levels, step, 0)
    spots = own_slots(holder[...], me, stream.shape[0])
    held = jnp.zeros((2 * width, stream.shape[0]), F32)
    for n in range(stages):
        field = jnp.concatenate(two_parts(sall[n].reshape(width, tile)), axis=0)
        held = held + lax.dot_general(field, spots[:, n * tile : (n + 1) * tile], NT, preferred_element_type=F32)
    held = (held[:width] + held[width:]).T
    count = jnp.sum((holder[...] == me).astype(F32), axis=1, keepdims=True).astype(jnp.int32)
    slot = lax.broadcasted_iota(jnp.int32, held.shape, 0)
    flow[...] = jnp.where(slot < count, held, stream[...])
    for r in range(levels):
        pltpu.make_async_copy(out.at[r], out_hbm.at[r], out_sem.at[r]).wait()


VMEM = pl.BlockSpec(memory_space=pltpu.VMEM)
HBM = pl.BlockSpec(memory_space=pltpu.HBM)
DMA = pltpu.SemaphoreType.DMA


def per_device(heat, lower, offset, share, holder, stream):
    levels, nodes, width = heat.shape
    cells = holder.shape[0]
    slots = stream.shape[0]
    holder = holder.reshape(1, cells)
    angle = math.pi * (np.arange(nodes, dtype=np.float32) + np.float32(0.5)) / nodes
    sines = jnp.asarray(np.repeat((0.125 * np.sin(angle)).astype(np.float32)[:, None], width, axis=1))
    cosines = jnp.asarray(np.repeat((0.125 * np.cos(angle)).astype(np.float32)[:, None], width, axis=1))
    params = functools.partial(pltpu.CompilerParams, vmem_limit_bytes=40 << 20)

    rows = width // N_ROW
    parts = 12
    stages = 4
    tile = cells // stages
    both = lambda: DMA((stages, N_ROW))
    tv, pvt, vel, sall = pl.pallas_call(
        fused_kernel,
        out_shape=(
            jax.ShapeDtypeStruct((levels + 2, nodes, width), F32),
            jax.ShapeDtypeStruct((levels, width, nodes), F32),
            jax.ShapeDtypeStruct((4 * width, tile), BF16),
            jax.ShapeDtypeStruct((stages, N_ROW, rows, tile), F32),
        ),
        in_specs=[HBM] * 6,
        out_specs=(VMEM,) * 4,
        scratch_shapes=[
            pltpu.VMEM((levels, nodes), jnp.int32),
            pltpu.VMEM((levels, nodes), F32),
            pltpu.VMEM((levels, nodes), F32),
            pltpu.VMEM((1, cells), jnp.int32),
            pltpu.VMEM((slots, width), F32),
            pltpu.VMEM((width, cells), F32),
            pltpu.VMEM((levels, 4 * width, nodes), BF16),
            pltpu.VMEM((stages, N_ROW, rows, tile), F32),
            pltpu.VMEM((stages, 2, 2, tile), F32),
            pltpu.VMEM((stages, 2, 2, tile), F32),
            pltpu.VMEM((stages, 2, rows, tile), F32),
            pltpu.VMEM((N_ROW, 1, 128), F32),
            pltpu.VMEM((stages, N_ROW, rows, tile), F32),
            pltpu.VMEM((N_ROW, 1, 128), F32),
            pltpu.VMEM((stages, rows, tile), F32),
            pltpu.VMEM((1, 128), F32),
            pltpu.VMEM((N_ROW, 1, 128), F32),
            pltpu.VMEM((width, 128), F32),
            pltpu.VMEM((width, 128), F32),
            pltpu.VMEM((4 * width, tile), BF16),
            DMA((levels,)), DMA((5,)),
            both(), both(), both(), both(),
            DMA((N_ROW,)), DMA((N_ROW,)), DMA((N_ROW,)), DMA((N_ROW,)),
            DMA((stages, 2)), DMA((stages, 2)), DMA((2, parts)), DMA((2, parts)),
        ],
        compiler_params=params(collective_id=0, has_side_effects=True),
        name="columns",
    )(*(pltpu.with_memory_space_constraint(x, pltpu.HBM) for x in (heat, lower, offset, share, holder, stream)))

    return pl.pallas_call(
        advance_kernel,
        out_shape=(jax.ShapeDtypeStruct(heat.shape, F32), jax.ShapeDtypeStruct((slots, width), F32)),
        in_specs=[VMEM] * 10,
        out_specs=(HBM, VMEM),
        scratch_shapes=[pltpu.VMEM((levels, nodes, width), F32), DMA((levels,))],
        compiler_params=params(),
        name="advance",
    )(tv, pvt, vel, sall, lower, offset, holder, stream, sines, cosines)


def solution(mesh):
    return jax.shard_map(
        per_device,
        mesh=mesh,
        in_specs=(P("row", None, "ma"), P("row", None), P("row", None), P("row", None), P(), P("row", "ma")),
        out_specs=(P("row", None, "ma"), P("row", "ma")),
        check_vma=False,
    )
```

```python
import functools
import math

import jax
import jax.numpy as jnp
import numpy as np
from jax import lax
from jax.experimental import pallas as pl
from jax.experimental.pallas import tpu as pltpu
from jax.sharding import PartitionSpec as P

MESH = pl.DeviceIdType.MESH
F32 = jnp.float32
BF16 = jnp.bfloat16
N_ROW = 16
N_MA = 16
HALO_PLAN = (2, 3, 4, 5, 6, 7, 8, 9, 10, 12)
NT = (((1,), (1,)), ((), ()))


def two_parts(x):
    hi = x.astype(BF16)
    return hi, (x - hi.astype(F32)).astype(BF16)


def one_hot(rows, first, index):
    at = lax.broadcasted_iota(jnp.int32, (rows, index.shape[1]), 0)
    return jnp.where(at == index - first, 1.0, 0.0).astype(BF16)


def geo_row(cells, first, count):
    c = (first + lax.broadcasted_iota(jnp.int32, (1, count), 1)).astype(F32)
    return 1.0 / (0.25 + (c + 0.5) / cells)


def own_slots(holder, me, slots):
    cells = holder.shape[1]
    start = jnp.sum((holder < me).astype(F32), axis=1, keepdims=True).astype(jnp.int32)
    c = lax.broadcasted_iota(jnp.int32, (1, cells), 1)
    return one_hot(slots, 0, jnp.where(holder == me, c - start, -1))


def fused_kernel(
    t_hbm, low_hbm, off_hbm, share_hbm, holder_hbm, stream_hbm, sin_hbm, cos_hbm,
    tv, pvt, vel_last, sall, slope,
    sines, cosines, low, off, share, holder, stream_in, stream, twt, sp, edge, rim, ends, rim_send, rs_buf, rim_buf, own, rim_own, eall, carry_up, carry_vel, vel,
    t_sem, in_sem, rs_send, rs_recv, ag_send, ag_recv, e_send, e_recv, ea_send, ea_recv, ma_send, ma_recv, h_send, h_recv,
):
    levels, width, nodes = pvt.shape
    cells = holder.shape[1]
    stages, tile = sp.shape[0], sp.shape[3]
    me = lax.axis_index("row")
    ma = lax.axis_index("ma")
    right, left = lax.rem(ma + 1, N_MA), lax.rem(ma + N_MA - 1, N_MA)
    parts = HALO_PLAN[-1]
    piece = nodes // parts

    small = [(holder_hbm, holder), (stream_hbm, stream_in), (share_hbm, share), (off_hbm, off), (low_hbm, low), (sin_hbm, sines), (cos_hbm, cosines)]
    loads = [pltpu.make_async_copy(src, dst, in_sem.at[k]) for k, (src, dst) in enumerate(small)]
    heat_loads = [pltpu.make_async_copy(t_hbm.at[r], tv.at[r + 1], t_sem.at[r]) for r in range(levels)]
    for copy in loads + heat_loads:
        copy.start()
    barrier = pltpu.get_barrier_semaphore()
    for d in range(1, N_ROW):
        pl.semaphore_signal(barrier, inc=1, device_id={"row": lax.rem(me + d, N_ROW)}, device_id_type=MESH)
    for side in (left, right):
        pl.semaphore_signal(barrier, inc=1, device_id={"ma": side}, device_id_type=MESH)

    @pl.when(me == 0)
    def _():
        tv[0] = jnp.zeros((nodes, width), F32)

    @pl.when(me == N_ROW - 1)
    def _():
        tv[levels + 1] = jnp.zeros((nodes, width), F32)

    for copy in loads[:5]:
        copy.wait()
    spots = own_slots(holder[...], me, stream_in.shape[0])
    placed = jnp.dot(jnp.concatenate(two_parts(stream_in[...].T), axis=0), spots, preferred_element_type=F32)
    stream[...] = placed[:width] + placed[width:]
    for r in range(levels):
        heat_loads[r].wait()
        weights = share[r : r + 1, :]
        offset = off[r : r + 1, :]
        heat = tv[r + 1].T
        for k, weight in enumerate((weights * (1.0 - offset), weights * offset)):
            hi, lo = two_parts(heat * weight)
            twt[r, 2 * k * width : (2 * k + 1) * width, :] = hi
            twt[r, (2 * k + 1) * width : (2 * k + 2) * width, :] = lo

    pl.semaphore_wait(barrier, N_ROW + 1)

    def to_row(src, dst, send, recv, peer):
        return pltpu.make_async_remote_copy(src_ref=src, dst_ref=dst, send_sem=send, recv_sem=recv, device_id={"row": peer}, device_id_type=MESH)

    def await_all(like, sem):
        pltpu.make_async_copy(like, like, sem).wait()

    def halo(side, k):
        peer = jnp.maximum(me - 1, 0) if side == 0 else jnp.minimum(me + 1, N_ROW - 1)
        at = pl.ds(k * piece, piece)
        mine, theirs = (1, levels + 1) if side == 0 else (levels, 0)
        return to_row(tv.at[mine, at], tv.at[theirs, at], h_send.at[side], h_recv.at[side], peer)

    def halo_start(first, last):
        for side, there in ((0, me > 0), (1, me < N_ROW - 1)):

            @pl.when(there)
            def _(side=side):
                for k in range(first, last):
                    halo(side, k).start()

    def pieces(n):
        return (2 * n, 2 * n + 1, 8 + 2 * n, 8 + 2 * n + 1)

    def rim_copies(n):
        return [
            pltpu.make_async_remote_copy(src_ref=edge.at[n, k], dst_ref=rim.at[n, k], send_sem=ma_send.at[n, k], recv_sem=ma_recv.at[n, k], device_id={"ma": side}, device_id_type=MESH)
            for k, side in enumerate((left, right))
        ]

    def rs_copy(n, d, src):
        return to_row(src, rs_buf.at[n, d], rs_send, rs_recv.at[n], lax.rem(me + d, N_ROW))

    def ag_copy(n, d):
        return to_row(own.at[n], sall.at[n, me], ag_send, ag_recv.at[n], lax.rem(me + d, N_ROW))

    def e_copy(p, d):
        return to_row(rim_send.at[p], rim_buf.at[d], e_send, e_recv, p)

    def ea_copy(d):
        return to_row(rim_own, eall.at[me], ea_send, ea_recv.at[lax.rem(me, 8) // 2], lax.rem(me + d, N_ROW))

    def sum_columns(n):
        sums = [jnp.zeros((4 * width, tile), F32)] * 2
        for r in range(levels):
            marks = one_hot(tile, n * tile, low[r : r + 1, :])
            sums[r % 2] = sums[r % 2] + lax.dot_general(twt[r], marks, NT, preferred_element_type=F32)
        half = 2 * width
        here, following = (0.25 * geo_row(cells, n * tile + k, tile) for k in range(2))
        lower = here * sums[0][:half] + here * sums[1][:half]
        lower = lower[:width] + lower[width:]
        upper = following * sums[0][half:] + following * sums[1][half:]
        upper = pltpu.roll(upper[:width] + upper[width:], 1, axis=1)
        lane = lax.broadcasted_iota(jnp.int32, (width, 128), 1)
        before = jnp.zeros((width, 128), F32) if n == 0 else carry_up[...]
        carry_up[...] = upper[:, :128]
        upper = jnp.concatenate([jnp.where(lane == 0, before, upper[:, :128]), upper[:, 128:]], axis=1)
        zint = lower + upper
        zero = jnp.zeros((1, tile), F32)
        ahead = jnp.concatenate([zint[1:], zero], axis=0)
        behind = jnp.concatenate([zero, zint[:-1]], axis=0)
        partial = stream[:, n * tile : (n + 1) * tile] - (ahead - behind)
        sp[n] = partial.reshape(N_ROW, width // N_ROW, tile)
        edge[n, 0] = jnp.concatenate([zint[:1], partial[:1]], axis=0)
        edge[n, 1] = jnp.concatenate([zint[-1:], partial[-1:]], axis=0)

    def send_inner(n):
        for copy in rim_copies(n):
            copy.start()
        for d in range(1, N_ROW):
            peer = lax.rem(me + d, N_ROW)

            @pl.when(jnp.logical_and(peer > 0, peer < N_ROW - 1))
            def _(d=d, peer=peer):
                rs_copy(n, d, sp.at[n, peer]).start()

    def send_outer(n):
        for copy in rim_copies(n):
            copy.wait()
        last = width // N_ROW - 1
        ends[n, 0] = sp[n, 0]
        ends[n, 1] = sp[n, N_ROW - 1]
        ends[n, 0, 0:1] = sp[n, 0, 0:1] + rim[n, 1, 0:1]
        ends[n, 1, last : last + 1] = sp[n, N_ROW - 1, last : last + 1] - rim[n, 0, 0:1]
        outer = (rim[n, 1, 1:2] - edge[n, 0, 0:1], rim[n, 0, 1:2] + edge[n, 1, 0:1])
        for i, p in enumerate(pieces(n)):
            rim_send[p] = outer[i // 2][:, (i % 2) * 128 : (i % 2 + 1) * 128]
        for k, p in enumerate((0, N_ROW - 1)):

            @pl.when(me != p)
            def _(k=k, p=p):
                rs_copy(n, lax.rem(p - me + N_ROW, N_ROW), ends.at[n, k]).start()

        for p in pieces(n):

            @pl.when(me != p)
            def _(p=p):
                e_copy(p, lax.rem(p - me + N_ROW, N_ROW)).start()

    def reduce_rows(n):
        total = jnp.where(me == 0, ends[n, 0], jnp.where(me == N_ROW - 1, ends[n, 1], sp[n, me]))
        await_all(rs_buf.at[n, pl.ds(1, N_ROW - 1)], rs_recv.at[n])
        for d in range(1, N_ROW):
            total = total + rs_buf[n, d]
        own[n] = total
        sall[n, me] = total
        for d in range(1, N_ROW):
            ag_copy(n, d).start()

        @pl.when(lax.rem(me, 8) // 2 == n)
        def _():
            total = rim_send[me]
            await_all(rim_buf.at[pl.ds(1, N_ROW - 1)], e_recv)
            for d in range(1, N_ROW):
                total = total + rim_buf[d]
            rim_own[...] = total
            eall[me] = total
            for d in range(1, N_ROW):
                ea_copy(d).start()

    def velocity(n):
        await_all(sall.at[n, pl.ds(1, N_ROW - 1)], ag_recv.at[n])
        mine = lax.rem(me, 8) // 2 == n
        for there, count in ((mine, 3), (jnp.logical_not(mine), 4)):

            @pl.when(there)
            def _(count=count):
                await_all(eall.at[pl.ds(0, count)], ea_recv.at[n])

        field = sall[n].reshape(width, tile)
        first, last = (jnp.concatenate([eall[p], eall[p + 1]], axis=1) for p in (2 * n, 8 + 2 * n))
        ahead = jnp.concatenate([field[1:], last], axis=0)
        behind = jnp.concatenate([first, field[:-1]], axis=0)
        now = (0.5 * geo_row(cells, n * tile, tile)) * (ahead - behind)
        lane = lax.broadcasted_iota(jnp.int32, (width, 128), 1)
        down = pltpu.roll(now, 1, axis=1)
        before = jnp.zeros((width, 128), F32) if n == 0 else carry_vel[...]
        carry_vel[...] = down[:, :128]
        down = jnp.concatenate([jnp.where(lane == 0, before, down[:, :128]), down[:, 128:]], axis=1)
        into = vel_last if n == stages - 1 else vel
        for k, x in enumerate(two_parts(down) + two_parts(now - down)):
            into[k * width : (k + 1) * width, :] = x

    def interpolate(n):
        def step(some, carry):
            for i in range(4 * (nodes // 256)):
                r, k = some * 4 + i // (nodes // 256), i % (nodes // 256)
                at = slice(k * 256, (k + 1) * 256)
                marks = one_hot(tile, n * tile - 1, low[pl.ds(r, 1), at])
                both = jnp.dot(vel[...], marks, preferred_element_type=F32)
                part = both[:width] + both[width : 2 * width]
                part = part + off[pl.ds(r, 1), at] * (both[2 * width : 3 * width] + both[3 * width :])
                pvt[r, :, at] = part if n == 0 else pvt[r, :, at] + part
            return carry

        lax.fori_loop(0, levels // 4, step, 0)

    def slopes(r):
        center = tv[r + 1]
        zero = jnp.zeros((1, width), F32)
        polar = jnp.concatenate([center[1:], zero], axis=0) - jnp.concatenate([zero, center[:-1]], axis=0)
        slope[r] = sines[...] * (tv[r + 2] - tv[r]) + cosines[...] * polar

    def finish():
        for side, there, comes in ((0, me > 0, me < N_ROW - 1), (1, me < N_ROW - 1, me > 0)):

            @pl.when(there)
            def _(side=side):
                await_all(tv.at[0], h_send.at[side])

            @pl.when(comes)
            def _(side=side):
                await_all(tv.at[0], h_recv.at[side])

    plan = iter(zip((0,) + HALO_PLAN, HALO_PLAN))
    halo_start(*next(plan))
    for n in range(stages):
        sum_columns(n)
        send_inner(n)
        if n > 0:
            send_outer(n - 1)
        halo_start(*next(plan))
    send_outer(stages - 1)
    halo_start(*next(plan))
    for copy in loads[5:]:
        copy.wait()
    for r in range(1, levels - 1):
        slopes(r)
    for n in range(stages):
        reduce_rows(n)
        halo_start(*next(plan))
    for n in range(stages - 1):
        velocity(n)
        interpolate(n)
    finish()
    slopes(0)
    slopes(levels - 1)
    velocity(stages - 1)
    for sem in (rs_send, ag_send):
        await_all(rs_buf.at[:, pl.ds(1, N_ROW - 1)], sem)
    for sem in (e_send, ea_send):
        await_all(rim_buf.at[pl.ds(1, N_ROW - 1)], sem)


def advance_kernel(tv, pvt, vel, sall, slope, low, off, holder, stream, out_hbm, flow, drift, out, out_sem):
    levels, nodes, width = out.shape
    cells = holder.shape[1]
    stages, tile = sall.shape[0], sall.shape[3]
    me = lax.axis_index("row")

    def interpolate(r):
        for k in range(nodes // 256):
            at = slice(k * 256, (k + 1) * 256)
            marks = one_hot(tile, (stages - 1) * tile - 1, low[pl.ds(r, 1), at])
            both = jnp.dot(vel[...], marks, preferred_element_type=F32)
            part = pvt[r, :, at] + both[:width] + both[width : 2 * width]
            drift[lax.rem(r, 2), :, at] = part + off[pl.ds(r, 1), at] * (both[2 * width : 3 * width] + both[3 * width :])

    def update(r):
        out[r] = tv[r + 1] - drift[lax.rem(r, 2)].T * slope[r]
        pltpu.make_async_copy(out.at[r], out_hbm.at[r], out_sem.at[r]).start()

    def step(r, carry):
        update(r - 1)
        interpolate(r)
        return carry

    interpolate(0)
    lax.fori_loop(1, levels, step, 0)
    update(levels - 1)
    spots = own_slots(holder[...], me, stream.shape[0])
    held = jnp.zeros((2 * width, stream.shape[0]), F32)
    for n in range(stages):
        field = jnp.concatenate(two_parts(sall[n].reshape(width, tile)), axis=0)
        held = held + lax.dot_general(field, spots[:, n * tile : (n + 1) * tile], NT, preferred_element_type=F32)
    held = (held[:width] + held[width:]).T
    count = jnp.sum((holder[...] == me).astype(F32), axis=1, keepdims=True).astype(jnp.int32)
    slot = lax.broadcasted_iota(jnp.int32, held.shape, 0)
    flow[...] = jnp.where(slot < count, held, stream[...])
    for r in range(levels):
        pltpu.make_async_copy(out.at[r], out_hbm.at[r], out_sem.at[r]).wait()


VMEM = pl.BlockSpec(memory_space=pltpu.VMEM)
HBM = pl.BlockSpec(memory_space=pltpu.HBM)
DMA = pltpu.SemaphoreType.DMA


def per_device(heat, lower, offset, share, holder, stream):
    levels, nodes, width = heat.shape
    cells = holder.shape[0]
    slots = stream.shape[0]
    holder = holder.reshape(1, cells)
    angle = math.pi * (np.arange(nodes, dtype=np.float32) + np.float32(0.5)) / nodes
    sines = jnp.asarray(np.repeat((0.125 * np.sin(angle)).astype(np.float32)[:, None], width, axis=1))
    cosines = jnp.asarray(np.repeat((0.125 * np.cos(angle)).astype(np.float32)[:, None], width, axis=1))
    params = functools.partial(pltpu.CompilerParams, vmem_limit_bytes=40 << 20)

    rows = width // N_ROW
    stages = 4
    tile = cells // stages
    tv, pvt, vel, sall, slope = pl.pallas_call(
        fused_kernel,
        out_shape=(
            jax.ShapeDtypeStruct((levels + 2, nodes, width), F32),
            jax.ShapeDtypeStruct((levels, width, nodes), F32),
            jax.ShapeDtypeStruct((4 * width, tile), BF16),
            jax.ShapeDtypeStruct((stages, N_ROW, rows, tile), F32),
            jax.ShapeDtypeStruct((levels, nodes, width), F32),
        ),
        in_specs=[HBM] * 8,
        out_specs=(VMEM,) * 5,
        scratch_shapes=[
            pltpu.VMEM((nodes, width), F32),
            pltpu.VMEM((nodes, width), F32),
            pltpu.VMEM((levels, nodes), jnp.int32),
            pltpu.VMEM((levels, nodes), F32),
            pltpu.VMEM((levels, nodes), F32),
            pltpu.VMEM((1, cells), jnp.int32),
            pltpu.VMEM((slots, width), F32),
            pltpu.VMEM((width, cells), F32),
            pltpu.VMEM((levels, 4 * width, nodes), BF16),
            pltpu.VMEM((stages, N_ROW, rows, tile), F32),
            pltpu.VMEM((stages, 2, 2, tile), F32),
            pltpu.VMEM((stages, 2, 2, tile), F32),
            pltpu.VMEM((stages, 2, rows, tile), F32),
            pltpu.VMEM((N_ROW, 1, 128), F32),
            pltpu.VMEM((stages, N_ROW, rows, tile), F32),
            pltpu.VMEM((N_ROW, 1, 128), F32),
            pltpu.VMEM((stages, rows, tile), F32),
            pltpu.VMEM((1, 128), F32),
            pltpu.VMEM((N_ROW, 1, 128), F32),
            pltpu.VMEM((width, 128), F32),
            pltpu.VMEM((width, 128), F32),
            pltpu.VMEM((4 * width, tile), BF16),
            DMA((levels,)), DMA((7,)),
            DMA, DMA((stages,)), DMA, DMA((stages,)),
            DMA, DMA, DMA, DMA((stages,)),
            DMA((stages, 2)), DMA((stages, 2)), DMA((2,)), DMA((2,)),
        ],
        compiler_params=params(collective_id=0, has_side_effects=True),
        name="columns",
    )(*(pltpu.with_memory_space_constraint(x, pltpu.HBM) for x in (heat, lower, offset, share, holder, stream, sines, cosines)))

    return pl.pallas_call(
        advance_kernel,
        out_shape=(jax.ShapeDtypeStruct(heat.shape, F32), jax.ShapeDtypeStruct((slots, width), F32)),
        in_specs=[VMEM] * 9,
        out_specs=(HBM, VMEM),
        scratch_shapes=[pltpu.VMEM((2, width, nodes), F32), pltpu.VMEM((levels, nodes, width), F32), DMA((levels,))],
        compiler_params=params(),
        name="advance",
    )(tv, pvt, vel, sall, slope, lower, offset, holder, stream)


def solution(mesh):
    return jax.shard_map(
        per_device,
        mesh=mesh,
        in_specs=(P("row", None, "ma"), P("row", None), P("row", None), P("row", None), P(), P("row", "ma")),
        out_specs=(P("row", None, "ma"), P("row", "ma")),
        check_vma=False,
    )
```

```python
import functools
import math

import jax
import jax.numpy as jnp
import numpy as np
from jax import lax
from jax.experimental import pallas as pl
from jax.experimental.pallas import tpu as pltpu
from jax.sharding import PartitionSpec as P

MESH = pl.DeviceIdType.MESH
F32 = jnp.float32
BF16 = jnp.bfloat16
N_ROW = 16
N_PAIR = 8
N_MA = 16
HALO_PLAN = (2, 3, 4, 4, 5, 7, 8, 9, 10, 12)
Y_LAST = (0, 1, 2, 3)
NT = (((1,), (1,)), ((), ()))


def two_parts(x):
    hi = x.astype(BF16)
    return hi, (x - hi.astype(F32)).astype(BF16)


def one_hot(rows, first, index):
    at = lax.broadcasted_iota(jnp.int32, (rows, index.shape[1]), 0)
    return jnp.where(at == index - first, 1.0, 0.0).astype(BF16)


def geo_row(cells, first, count):
    c = (first + lax.broadcasted_iota(jnp.int32, (1, count), 1)).astype(F32)
    return 1.0 / (0.25 + (c + 0.5) / cells)


def by_azimuth(gathered, n):
    half, pairs, rows, tile = gathered.shape[1:]
    return jnp.stack([gathered[n, k] for k in range(half)], axis=1).reshape(half * pairs * rows, tile)


def own_slots(holder, me, slots):
    cells = holder.shape[1]
    start = jnp.sum((holder < me).astype(F32), axis=1, keepdims=True).astype(jnp.int32)
    c = lax.broadcasted_iota(jnp.int32, (1, cells), 1)
    return one_hot(slots, 0, jnp.where(holder == me, c - start, -1))


def fused_kernel(
    t_hbm, low_hbm, off_hbm, share_hbm, holder_hbm, stream_hbm, sin_hbm, cos_hbm,
    tv, pvt, vel_last, sall, slope,
    sines, cosines, low, off, share, holder, stream_in, stream, twt, sp, pair_in, pair, edge, rim, fix, fix_in, rim_send, rs_buf, rim_buf, own, rim_own, eall, carry_up, carry_vel, vel,
    t_sem, in_sem, y_send, y_recv, fix_send, fix_recv, rs_send, rs_recv, ag_send, ag_recv, agy_send, agy_recv, e_send, e_recv, ea_send, ea_recv, ma_send, ma_recv, h_send, h_recv,
):
    levels, width, nodes = pvt.shape
    cells = holder.shape[1]
    stages, tile = sp.shape[0], sp.shape[4]
    me = lax.axis_index("row")
    side_y, at_z = lax.rem(me, 2), me // 2
    partner = me + 1 - 2 * side_y
    ma = lax.axis_index("ma")
    right, left = lax.rem(ma + 1, N_MA), lax.rem(ma + N_MA - 1, N_MA)
    parts = HALO_PLAN[-1]
    piece = nodes // parts

    small = [(holder_hbm, holder), (stream_hbm, stream_in), (share_hbm, share), (off_hbm, off), (low_hbm, low), (sin_hbm, sines), (cos_hbm, cosines)]
    loads = [pltpu.make_async_copy(src, dst, in_sem.at[k]) for k, (src, dst) in enumerate(small)]
    heat_loads = [pltpu.make_async_copy(t_hbm.at[r], tv.at[r + 1], t_sem.at[r]) for r in range(levels)]
    for copy in loads + heat_loads:
        copy.start()
    barrier = pltpu.get_barrier_semaphore()
    for d in range(1, N_ROW):
        pl.semaphore_signal(barrier, inc=1, device_id={"row": lax.rem(me + d, N_ROW)}, device_id_type=MESH)
    for side in (left, right):
        pl.semaphore_signal(barrier, inc=1, device_id={"ma": side}, device_id_type=MESH)

    @pl.when(me == 0)
    def _():
        tv[0] = jnp.zeros((nodes, width), F32)

    @pl.when(me == N_ROW - 1)
    def _():
        tv[levels + 1] = jnp.zeros((nodes, width), F32)

    for copy in loads[:5]:
        copy.wait()
    spots = own_slots(holder[...], me, stream_in.shape[0])
    placed = jnp.dot(jnp.concatenate(two_parts(stream_in[...].T), axis=0), spots, preferred_element_type=F32)
    stream[...] = placed[:width] + placed[width:]

    def prepare(r):
        weights = share[r : r + 1, :]
        offset = off[r : r + 1, :]
        heat = tv[r + 1].T
        for k, weight in enumerate((weights * (1.0 - offset), weights * offset)):
            hi, lo = two_parts(heat * weight)
            twt[r, 2 * k * width : (2 * k + 1) * width, :] = hi
            twt[r, (2 * k + 1) * width : (2 * k + 2) * width, :] = lo


    def to_row(src, dst, send, recv, peer):
        return pltpu.make_async_remote_copy(src_ref=src, dst_ref=dst, send_sem=send, recv_sem=recv, device_id={"row": peer}, device_id_type=MESH)

    def await_all(like, sem):
        pltpu.make_async_copy(like, like, sem).wait()

    def halo(side, k):
        peer = jnp.maximum(me - 1, 0) if side == 0 else jnp.minimum(me + 1, N_ROW - 1)
        at = pl.ds(k * piece, piece)
        mine, theirs = (1, levels + 1) if side == 0 else (levels, 0)
        return to_row(tv.at[mine, at], tv.at[theirs, at], h_send.at[side], h_recv.at[side], peer)

    def halo_start(first, last):
        for side, there in ((0, me > 0), (1, me < N_ROW - 1)):

            @pl.when(there)
            def _(side=side):
                for k in range(first, last):
                    halo(side, k).start()

    def pieces(n):
        return (2 * n, 2 * n + 1, 8 + 2 * n, 8 + 2 * n + 1)

    def rim_copies(n):
        return [
            pltpu.make_async_remote_copy(src_ref=edge.at[n, k], dst_ref=rim.at[n, k], send_sem=ma_send.at[n, k], recv_sem=ma_recv.at[n, k], device_id={"ma": side}, device_id_type=MESH)
            for k, side in enumerate((left, right))
        ]

    def y_copy(n):
        return to_row(sp.at[n, 1 - side_y], pair_in.at[n], y_send, y_recv.at[n], partner)

    def rs_copy(n, dz):
        z = lax.rem(at_z + dz, N_PAIR)
        return to_row(pair.at[n, z], rs_buf.at[n, dz], rs_send, rs_recv.at[n], 2 * z + side_y)

    def fix_copy(n, k, p):
        d = lax.rem(p - me + N_ROW, N_ROW)
        return to_row(fix.at[n, k], fix_in.at[n, d], fix_send, fix_recv.at[n], p)

    def gather_first(n):
        if n in Y_LAST:
            peers = [2 * lax.rem(at_z + dz, N_PAIR) + side_y for dz in range(1, N_PAIR)]
        else:
            peers = [lax.rem(me + d, N_ROW) for d in range(1, N_ROW)]
        for peer in peers:
            to_row(own.at[n], sall.at[n, side_y, at_z], ag_send.at[n], ag_recv.at[n], peer).start()

    def forward(n):
        if n in Y_LAST:
            await_all(rs_buf.at[n, pl.ds(1, N_PAIR - 1)], ag_recv.at[n])
            to_row(sall.at[n, side_y], sall.at[n, side_y], agy_send.at[n], agy_recv.at[n], partner).start()

    def await_gathered(n):
        if n in Y_LAST:
            await_all(pair.at[n], agy_recv.at[n])
        else:
            await_all(rs_buf.at[pl.ds(0, 3), pl.ds(0, 5)], ag_recv.at[n])

    def await_sent(n):
        if n in Y_LAST:
            await_all(rs_buf.at[n, pl.ds(1, N_PAIR - 1)], ag_send.at[n])
            await_all(pair.at[n], agy_send.at[n])
        else:
            await_all(rs_buf.at[pl.ds(0, 3), pl.ds(0, 5)], ag_send.at[n])

    def e_copy(p, d):
        return to_row(rim_send.at[p], rim_buf.at[d], e_send, e_recv, p)

    def ea_copy(d):
        return to_row(rim_own, eall.at[me], ea_send, ea_recv.at[lax.rem(me, 8) // 2], lax.rem(me + d, N_ROW))

    def sum_columns(n):
        sums = [jnp.zeros((4 * width, tile), F32)] * 2
        for r in range(levels):
            if n == 0:
                if r % 4 == 0:
                    for copy in heat_loads[r : r + 4]:
                        copy.wait()
                if r == 4:
                    pl.semaphore_wait(barrier, N_ROW + 1)
                    halo_start(*next(plan))
                prepare(r)
            marks = one_hot(tile, n * tile, low[r : r + 1, :])
            sums[r % 2] = sums[r % 2] + lax.dot_general(twt[r], marks, NT, preferred_element_type=F32)
        half = 2 * width
        here, following = (0.25 * geo_row(cells, n * tile + k, tile) for k in range(2))
        lower = here * sums[0][:half] + here * sums[1][:half]
        lower = lower[:width] + lower[width:]
        upper = following * sums[0][half:] + following * sums[1][half:]
        upper = pltpu.roll(upper[:width] + upper[width:], 1, axis=1)
        lane = lax.broadcasted_iota(jnp.int32, (width, 128), 1)
        before = jnp.zeros((width, 128), F32) if n == 0 else carry_up[...]
        carry_up[...] = upper[:, :128]
        upper = jnp.concatenate([jnp.where(lane == 0, before, upper[:, :128]), upper[:, 128:]], axis=1)
        zint = lower + upper
        zero = jnp.zeros((1, tile), F32)
        ahead = jnp.concatenate([zint[1:], zero], axis=0)
        behind = jnp.concatenate([zero, zint[:-1]], axis=0)
        partial = stream[:, n * tile : (n + 1) * tile] - (ahead - behind)
        chunks = partial.reshape(N_PAIR, 2, width // N_ROW, tile)
        for k in range(2):
            sp[n, k] = chunks[:, k]
        edge[n, 0] = jnp.concatenate([zint[:1], partial[:1]], axis=0)
        edge[n, 1] = jnp.concatenate([zint[-1:], partial[-1:]], axis=0)

    def send_inner(n):
        for copy in rim_copies(n):
            copy.start()
        y_copy(n).start()

    def send_outer(n):
        for copy in rim_copies(n):
            copy.wait()
        fix[n, 0] = rim[n, 1, 0:1]
        fix[n, 1] = rim[n, 0, 0:1]
        outer = (rim[n, 1, 1:2] - edge[n, 0, 0:1], rim[n, 0, 1:2] + edge[n, 1, 0:1])
        for i, p in enumerate(pieces(n)):
            rim_send[p] = outer[i // 2][:, (i % 2) * 128 : (i % 2 + 1) * 128]
        for k, p in enumerate((0, N_ROW - 1)):

            @pl.when(me != p)
            def _(k=k, p=p):
                fix_copy(n, k, p).start()

        for p in pieces(n):

            @pl.when(me != p)
            def _(p=p):
                e_copy(p, lax.rem(p - me + N_ROW, N_ROW)).start()

    def pair_rows(n):
        await_all(pair_in.at[n], y_recv.at[n])
        pair[n] = sp[n, side_y] + pair_in[n]
        for dz in range(1, N_PAIR):
            rs_copy(n, dz).start()

    def reduce_rows(n):
        await_all(rs_buf.at[n, pl.ds(1, N_PAIR - 1)], rs_recv.at[n])
        total = pair[n, at_z]
        for dz in range(1, N_PAIR):
            total = total + rs_buf[n, dz]
        own[n] = total
        for k, (p, at, sign) in enumerate(((0, 0, 1.0), (N_ROW - 1, width // N_ROW - 1, -1.0))):

            @pl.when(me == p)
            def _(k=k, at=at, sign=sign):
                await_all(fix_in.at[n, pl.ds(1, N_ROW - 1)], fix_recv.at[n])
                more = fix[n, k]
                for d in range(1, N_ROW):
                    more = more + fix_in[n, d]
                own[n, at : at + 1] = own[n, at : at + 1] + sign * more

        sall[n, side_y, at_z] = own[n]
        gather_first(n)

        @pl.when(lax.rem(me, 8) // 2 == n)
        def _():
            total = rim_send[me]
            await_all(rim_buf.at[pl.ds(1, N_ROW - 1)], e_recv)
            for d in range(1, N_ROW):
                total = total + rim_buf[d]
            rim_own[...] = total
            eall[me] = total
            for d in range(1, N_ROW):
                ea_copy(d).start()

    def velocity(n):
        await_gathered(n)
        mine = lax.rem(me, 8) // 2 == n
        for there, count in ((mine, 3), (jnp.logical_not(mine), 4)):

            @pl.when(there)
            def _(count=count):
                await_all(eall.at[pl.ds(0, count)], ea_recv.at[n])

        field = by_azimuth(sall, n)
        first, last = (jnp.concatenate([eall[p], eall[p + 1]], axis=1) for p in (2 * n, 8 + 2 * n))
        ahead = jnp.concatenate([field[1:], last], axis=0)
        behind = jnp.concatenate([first, field[:-1]], axis=0)
        now = (0.5 * geo_row(cells, n * tile, tile)) * (ahead - behind)
        lane = lax.broadcasted_iota(jnp.int32, (width, 128), 1)
        down = pltpu.roll(now, 1, axis=1)
        before = jnp.zeros((width, 128), F32) if n == 0 else carry_vel[...]
        carry_vel[...] = down[:, :128]
        down = jnp.concatenate([jnp.where(lane == 0, before, down[:, :128]), down[:, 128:]], axis=1)
        into = vel_last if n == stages - 1 else vel
        for k, x in enumerate(two_parts(down) + two_parts(now - down)):
            into[k * width : (k + 1) * width, :] = x

    def interpolate(n):
        def step(some, carry):
            for i in range(4 * (nodes // 256)):
                r, k = some * 4 + i // (nodes // 256), i % (nodes // 256)
                at = slice(k * 256, (k + 1) * 256)
                marks = one_hot(tile, n * tile - 1, low[pl.ds(r, 1), at])
                both = jnp.dot(vel[...], marks, preferred_element_type=F32)
                part = both[:width] + both[width : 2 * width]
                part = part + off[pl.ds(r, 1), at] * (both[2 * width : 3 * width] + both[3 * width :])
                pvt[r, :, at] = part if n == 0 else pvt[r, :, at] + part
            return carry

        lax.fori_loop(0, levels // 4, step, 0)

    def slopes(r):
        center = tv[r + 1]
        zero = jnp.zeros((1, width), F32)
        polar = jnp.concatenate([center[1:], zero], axis=0) - jnp.concatenate([zero, center[:-1]], axis=0)
        slope[r] = sines[...] * (tv[r + 2] - tv[r]) + cosines[...] * polar

    def finish():
        for side, there, comes in ((0, me > 0, me < N_ROW - 1), (1, me < N_ROW - 1, me > 0)):

            @pl.when(there)
            def _(side=side):
                await_all(tv.at[0], h_send.at[side])

            @pl.when(comes)
            def _(side=side):
                await_all(tv.at[0], h_recv.at[side])

    plan = iter(zip((0,) + HALO_PLAN, HALO_PLAN))
    for n in range(stages):
        sum_columns(n)
        send_inner(n)
        if n > 0:
            send_outer(n - 1)
        if n > 1:
            pair_rows(n - 2)
        halo_start(*next(plan))
    for copy in loads[5:]:
        copy.wait()
    for r in range(1, levels - 1):
        slopes(r)
    pair_rows(2)
    reduce_rows(0)
    send_outer(3)
    halo_start(*next(plan))
    pair_rows(3)
    halo_start(*next(plan))
    reduce_rows(1)
    halo_start(*next(plan))
    forward(0)
    reduce_rows(2)
    halo_start(*next(plan))
    reduce_rows(3)
    forward(1)
    halo_start(*next(plan))
    velocity(0)
    interpolate(0)
    forward(2)
    velocity(1)
    forward(3)
    interpolate(1)
    velocity(2)
    interpolate(2)
    finish()
    slopes(0)
    slopes(levels - 1)
    velocity(stages - 1)
    await_all(pair_in, y_send)
    await_all(rs_buf.at[:, pl.ds(1, N_PAIR - 1)], rs_send)
    for n in range(stages):
        await_sent(n)
    inner = jnp.logical_and(me > 0, me < N_ROW - 1)
    for there, count in ((inner, 8), (jnp.logical_not(inner), 4)):

        @pl.when(there)
        def _(count=count):
            await_all(fix_in.at[0, pl.ds(0, count)], fix_send)

    for sem in (e_send, ea_send):
        await_all(rim_buf.at[pl.ds(1, N_ROW - 1)], sem)


def advance_kernel(tv, pvt, vel, sall, slope, low, off, holder, stream, out_hbm, flow, drift, out, out_sem):
    levels, nodes, width = out.shape
    cells = holder.shape[1]
    stages, tile = sall.shape[0], sall.shape[4]
    me = lax.axis_index("row")

    def blend(r):
        for k in range(nodes // 256):
            at = slice(k * 256, (k + 1) * 256)
            marks = one_hot(tile, (stages - 1) * tile - 1, low[pl.ds(r, 1), at])
            both = jnp.dot(vel[...], marks, preferred_element_type=F32)
            part = pvt[r, :, at] + both[:width] + both[width : 2 * width]
            drift[lax.rem(r, 2), :, at] = part + off[pl.ds(r, 1), at] * (both[2 * width : 3 * width] + both[3 * width :])

    def update(r):
        out[r] = tv[r + 1] - drift[lax.rem(r, 2)].T * slope[r]
        pltpu.make_async_copy(out.at[r], out_hbm.at[r], out_sem.at[r]).start()

    def step(r, carry):
        update(r - 1)
        blend(r)
        return carry

    blend(0)
    lax.fori_loop(1, levels, step, 0, unroll=levels - 1)
    update(levels - 1)
    spots = own_slots(holder[...], me, stream.shape[0])
    held = jnp.zeros((2 * width, stream.shape[0]), F32)
    for n in range(stages):
        field = jnp.concatenate(two_parts(by_azimuth(sall, n)), axis=0)
        held = held + lax.dot_general(field, spots[:, n * tile : (n + 1) * tile], NT, preferred_element_type=F32)
    held = (held[:width] + held[width:]).T
    count = jnp.sum((holder[...] == me).astype(F32), axis=1, keepdims=True).astype(jnp.int32)
    slot = lax.broadcasted_iota(jnp.int32, held.shape, 0)
    flow[...] = jnp.where(slot < count, held, stream[...])
    for r in range(levels):
        pltpu.make_async_copy(out.at[r], out_hbm.at[r], out_sem.at[r]).wait()


VMEM = pl.BlockSpec(memory_space=pltpu.VMEM)
HBM = pl.BlockSpec(memory_space=pltpu.HBM)
DMA = pltpu.SemaphoreType.DMA


def per_device(heat, lower, offset, share, holder, stream):
    levels, nodes, width = heat.shape
    cells = holder.shape[0]
    slots = stream.shape[0]
    holder = holder.reshape(1, cells)
    angle = math.pi * (np.arange(nodes, dtype=np.float32) + np.float32(0.5)) / nodes
    sines = jnp.asarray(np.repeat((0.125 * np.sin(angle)).astype(np.float32)[:, None], width, axis=1))
    cosines = jnp.asarray(np.repeat((0.125 * np.cos(angle)).astype(np.float32)[:, None], width, axis=1))
    params = functools.partial(pltpu.CompilerParams, vmem_limit_bytes=40 << 20)

    rows = width // N_ROW
    stages = 4
    tile = cells // stages
    tv, pvt, vel, sall, slope = pl.pallas_call(
        fused_kernel,
        out_shape=(
            jax.ShapeDtypeStruct((levels + 2, nodes, width), F32),
            jax.ShapeDtypeStruct((levels, width, nodes), F32),
            jax.ShapeDtypeStruct((4 * width, tile), BF16),
            jax.ShapeDtypeStruct((stages, 2, N_PAIR, rows, tile), F32),
            jax.ShapeDtypeStruct((levels, nodes, width), F32),
        ),
        in_specs=[HBM] * 8,
        out_specs=(VMEM,) * 5,
        scratch_shapes=[
            pltpu.VMEM((nodes, width), F32),
            pltpu.VMEM((nodes, width), F32),
            pltpu.VMEM((levels, nodes), jnp.int32),
            pltpu.VMEM((levels, nodes), F32),
            pltpu.VMEM((levels, nodes), F32),
            pltpu.VMEM((1, cells), jnp.int32),
            pltpu.VMEM((slots, width), F32),
            pltpu.VMEM((width, cells), F32),
            pltpu.VMEM((levels, 4 * width, nodes), BF16),
            pltpu.VMEM((stages, 2, N_PAIR, rows, tile), F32),
            pltpu.VMEM((stages, N_PAIR, rows, tile), F32),
            pltpu.VMEM((stages, N_PAIR, rows, tile), F32),
            pltpu.VMEM((stages, 2, 2, tile), F32),
            pltpu.VMEM((stages, 2, 2, tile), F32),
            pltpu.VMEM((stages, 2, 1, tile), F32),
            pltpu.VMEM((stages, N_ROW, 1, tile), F32),
            pltpu.VMEM((N_ROW, 1, 128), F32),
            pltpu.VMEM((stages, N_PAIR, rows, tile), F32),
            pltpu.VMEM((N_ROW, 1, 128), F32),
            pltpu.VMEM((stages, rows, tile), F32),
            pltpu.VMEM((1, 128), F32),
            pltpu.VMEM((N_ROW, 1, 128), F32),
            pltpu.VMEM((width, 128), F32),
            pltpu.VMEM((width, 128), F32),
            pltpu.VMEM((4 * width, tile), BF16),
            DMA((levels,)), DMA((7,)),
            DMA, DMA((stages,)), DMA, DMA((stages,)),
            DMA, DMA((stages,)), DMA((stages,)), DMA((stages,)), DMA((stages,)), DMA((stages,)),
            DMA, DMA, DMA, DMA((stages,)),
            DMA((stages, 2)), DMA((stages, 2)), DMA((2,)), DMA((2,)),
        ],
        compiler_params=params(collective_id=0, has_side_effects=True),
        name="columns",
    )(*(pltpu.with_memory_space_constraint(x, pltpu.HBM) for x in (heat, lower, offset, share, holder, stream, sines, cosines)))

    return pl.pallas_call(
        advance_kernel,
        out_shape=(jax.ShapeDtypeStruct(heat.shape, F32), jax.ShapeDtypeStruct((slots, width), F32)),
        in_specs=[VMEM] * 9,
        out_specs=(HBM, VMEM),
        scratch_shapes=[pltpu.VMEM((2, width, nodes), F32), pltpu.VMEM((levels, nodes, width), F32), DMA((levels,))],
        compiler_params=params(),
        name="advance",
    )(tv, pvt, vel, sall, slope, lower, offset, holder, stream)


def solution(mesh):
    return jax.shard_map(
        per_device,
        mesh=mesh,
        in_specs=(P("row", None, "ma"), P("row", None), P("row", None), P("row", None), P(), P("row", "ma")),
        out_specs=(P("row", None, "ma"), P("row", "ma")),
        check_vma=False,
    )
```

```python
import functools
import math

import jax
import jax.numpy as jnp
import numpy as np
from jax import lax
from jax.experimental import pallas as pl
from jax.experimental.pallas import tpu as pltpu
from jax.sharding import PartitionSpec as P

MESH = pl.DeviceIdType.MESH
F32 = jnp.float32
BF16 = jnp.bfloat16
N_ROW = 16
N_PAIR = 8
N_MA = 16
HALO_PLAN = (2, 3, 3, 3, 5, 6, 7, 8, 9, 12)
Y_LAST = (0, 1)
NT = (((1,), (1,)), ((), ()))


def two_parts(x):
    hi = x.astype(BF16)
    return hi, (x - hi.astype(F32)).astype(BF16)


def one_hot(rows, first, index):
    at = lax.broadcasted_iota(jnp.int32, (rows, index.shape[1]), 0)
    return jnp.where(at == index - first, 1.0, 0.0).astype(BF16)


def geo_row(cells, first, count):
    c = (first + lax.broadcasted_iota(jnp.int32, (1, count), 1)).astype(F32)
    return 1.0 / (0.25 + (c + 0.5) / cells)


def by_azimuth(gathered, n):
    half, pairs, rows, tile = gathered.shape[1:]
    return jnp.stack([gathered[n, k] for k in range(half)], axis=1).reshape(half * pairs * rows, tile)


def own_slots(holder, me, slots):
    cells = holder.shape[1]
    start = jnp.sum((holder < me).astype(F32), axis=1, keepdims=True).astype(jnp.int32)
    c = lax.broadcasted_iota(jnp.int32, (1, cells), 1)
    return one_hot(slots, 0, jnp.where(holder == me, c - start, -1))


def fused_kernel(
    t_hbm, low_hbm, off_hbm, share_hbm, holder_hbm, stream_hbm, sin_hbm, cos_hbm,
    tv, pvt, vel_last, sall, slope,
    sines, cosines, low, off, share, holder, stream_in, stream, twt, sp, pair_in, pair, edge, rim, fix, fix_in, rim_send, rs_buf, rim_buf, own, rim_own, eall, carry_up, carry_vel, vel,
    t_sem, in_sem, y_send, y_recv, fix_send, fix_recv, rs_send, rs_recv, ag_send, ag_recv, agy_send, agy_recv, e_send, e_recv, ea_send, ea_recv, ma_send, ma_recv, h_send, h_recv,
):
    levels, width, nodes = pvt.shape
    cells = holder.shape[1]
    stages, tile = sp.shape[0], sp.shape[4]
    me = lax.axis_index("row")
    side_y, at_z = lax.rem(me, 2), me // 2
    partner = me + 1 - 2 * side_y
    ma = lax.axis_index("ma")
    right, left = lax.rem(ma + 1, N_MA), lax.rem(ma + N_MA - 1, N_MA)
    parts = HALO_PLAN[-1]
    piece = nodes // parts

    small = [(holder_hbm, holder), (stream_hbm, stream_in), (share_hbm, share), (off_hbm, off), (low_hbm, low), (sin_hbm, sines), (cos_hbm, cosines)]
    loads = [pltpu.make_async_copy(src, dst, in_sem.at[k]) for k, (src, dst) in enumerate(small)]
    heat_loads = [pltpu.make_async_copy(t_hbm.at[r], tv.at[r + 1], t_sem.at[r]) for r in range(levels)]
    for copy in loads + heat_loads:
        copy.start()
    barrier = pltpu.get_barrier_semaphore()
    for d in range(1, N_ROW):
        pl.semaphore_signal(barrier, inc=1, device_id={"row": lax.rem(me + d, N_ROW)}, device_id_type=MESH)
    for side in (left, right):
        pl.semaphore_signal(barrier, inc=1, device_id={"ma": side}, device_id_type=MESH)

    @pl.when(me == 0)
    def _():
        tv[0] = jnp.zeros((nodes, width), F32)

    @pl.when(me == N_ROW - 1)
    def _():
        tv[levels + 1] = jnp.zeros((nodes, width), F32)

    for copy in loads[:5]:
        copy.wait()
    spots = own_slots(holder[...], me, stream_in.shape[0])
    placed = jnp.dot(jnp.concatenate(two_parts(stream_in[...].T), axis=0), spots, preferred_element_type=F32)
    stream[...] = placed[:width] + placed[width:]

    def prepare(r):
        weights = share[r : r + 1, :]
        offset = off[r : r + 1, :]
        heat = tv[r + 1].T
        for k, weight in enumerate((weights * (1.0 - offset), weights * offset)):
            hi, lo = two_parts(heat * weight)
            twt[r, 2 * k * width : (2 * k + 1) * width, :] = hi
            twt[r, (2 * k + 1) * width : (2 * k + 2) * width, :] = lo


    def to_row(src, dst, send, recv, peer):
        return pltpu.make_async_remote_copy(src_ref=src, dst_ref=dst, send_sem=send, recv_sem=recv, device_id={"row": peer}, device_id_type=MESH)

    def await_all(like, sem):
        pltpu.make_async_copy(like, like, sem).wait()

    def halo(side, k):
        peer = jnp.maximum(me - 1, 0) if side == 0 else jnp.minimum(me + 1, N_ROW - 1)
        at = pl.ds(k * piece, piece)
        mine, theirs = (1, levels + 1) if side == 0 else (levels, 0)
        return to_row(tv.at[mine, at], tv.at[theirs, at], h_send.at[side], h_recv.at[side], peer)

    def halo_start(first, last):
        for side, there in ((0, me > 0), (1, me < N_ROW - 1)):

            @pl.when(there)
            def _(side=side):
                for k in range(first, last):
                    halo(side, k).start()

    def pieces(n):
        return (2 * n, 2 * n + 1, 8 + 2 * n, 8 + 2 * n + 1)

    def rim_copies(n):
        return [
            pltpu.make_async_remote_copy(src_ref=edge.at[n, k], dst_ref=rim.at[n, k], send_sem=ma_send.at[n, k], recv_sem=ma_recv.at[n, k], device_id={"ma": side}, device_id_type=MESH)
            for k, side in enumerate((left, right))
        ]

    def y_copy(n):
        return to_row(sp.at[n, 1 - side_y], pair_in.at[n], y_send, y_recv.at[n], partner)

    def rs_copy(n, dz):
        z = lax.rem(at_z + dz, N_PAIR)
        return to_row(pair.at[n, z], rs_buf.at[n, dz], rs_send, rs_recv.at[n], 2 * z + side_y)

    def fix_copy(n, k, p):
        d = lax.rem(p - me + N_ROW, N_ROW)
        return to_row(fix.at[n, k], fix_in.at[n, d], fix_send, fix_recv.at[n], p)

    def along_z(src, n, half):
        for dz in range(1, N_PAIR):
            peer = 2 * lax.rem(at_z + dz, N_PAIR) + side_y
            to_row(src, sall.at[n, half, at_z], ag_send.at[n], ag_recv.at[n], peer).start()

    def gather_first(n):
        if n not in Y_LAST:
            to_row(own.at[n], sall.at[n, side_y, at_z], agy_send.at[n], agy_recv.at[n], partner).start()
        along_z(own.at[n], n, side_y)

    def forward(n):
        if n in Y_LAST:
            await_all(rs_buf.at[n, pl.ds(1, N_PAIR - 1)], ag_recv.at[n])
            to_row(sall.at[n, side_y], sall.at[n, side_y], agy_send.at[n], agy_recv.at[n], partner).start()
        else:
            await_all(own.at[n], agy_recv.at[n])
            along_z(sall.at[n, 1 - side_y, at_z], n, 1 - side_y)

    def await_gathered(n):
        if n in Y_LAST:
            await_all(pair.at[n], agy_recv.at[n])
        else:
            await_all(rs_buf.at[pl.ds(0, 2), pl.ds(1, N_PAIR - 1)], ag_recv.at[n])

    def await_sent(n):
        if n in Y_LAST:
            await_all(rs_buf.at[n, pl.ds(1, N_PAIR - 1)], ag_send.at[n])
            await_all(pair.at[n], agy_send.at[n])
        else:
            await_all(rs_buf.at[pl.ds(0, 2), pl.ds(1, N_PAIR - 1)], ag_send.at[n])
            await_all(own.at[n], agy_send.at[n])

    def e_copy(p, d):
        return to_row(rim_send.at[p], rim_buf.at[d], e_send, e_recv, p)

    def ea_copy(d):
        return to_row(rim_own, eall.at[me], ea_send, ea_recv.at[lax.rem(me, 8) // 2], lax.rem(me + d, N_ROW))

    def sum_columns(n):
        sums = [jnp.zeros((4 * width, tile), F32)] * 2
        for r in range(levels):
            if n == 0:
                if r % 4 == 0:
                    for copy in heat_loads[r : r + 4]:
                        copy.wait()
                if r == 4:
                    pl.semaphore_wait(barrier, N_ROW + 1)
                    halo_start(*next(plan))
                prepare(r)
            marks = one_hot(tile, n * tile, low[r : r + 1, :])
            sums[r % 2] = sums[r % 2] + lax.dot_general(twt[r], marks, NT, preferred_element_type=F32)
        half = 2 * width
        here, following = (0.25 * geo_row(cells, n * tile + k, tile) for k in range(2))
        lower = here * sums[0][:half] + here * sums[1][:half]
        lower = lower[:width] + lower[width:]
        upper = following * sums[0][half:] + following * sums[1][half:]
        upper = pltpu.roll(upper[:width] + upper[width:], 1, axis=1)
        lane = lax.broadcasted_iota(jnp.int32, (width, 128), 1)
        before = jnp.zeros((width, 128), F32) if n == 0 else carry_up[...]
        carry_up[...] = upper[:, :128]
        upper = jnp.concatenate([jnp.where(lane == 0, before, upper[:, :128]), upper[:, 128:]], axis=1)
        zint = lower + upper
        zero = jnp.zeros((1, tile), F32)
        ahead = jnp.concatenate([zint[1:], zero], axis=0)
        behind = jnp.concatenate([zero, zint[:-1]], axis=0)
        partial = stream[:, n * tile : (n + 1) * tile] - (ahead - behind)
        chunks = partial.reshape(N_PAIR, 2, width // N_ROW, tile)
        for k in range(2):
            sp[n, k] = chunks[:, k]
        edge[n, 0] = jnp.concatenate([zint[:1], partial[:1]], axis=0)
        edge[n, 1] = jnp.concatenate([zint[-1:], partial[-1:]], axis=0)

    def send_inner(n):
        for copy in rim_copies(n):
            copy.start()
        y_copy(n).start()

    def send_outer(n):
        for copy in rim_copies(n):
            copy.wait()
        fix[n, 0] = rim[n, 1, 0:1]
        fix[n, 1] = rim[n, 0, 0:1]
        outer = (rim[n, 1, 1:2] - edge[n, 0, 0:1], rim[n, 0, 1:2] + edge[n, 1, 0:1])
        for i, p in enumerate(pieces(n)):
            rim_send[p] = outer[i // 2][:, (i % 2) * 128 : (i % 2 + 1) * 128]
        for k, p in enumerate((0, N_ROW - 1)):

            @pl.when(me != p)
            def _(k=k, p=p):
                fix_copy(n, k, p).start()

        for p in pieces(n):

            @pl.when(me != p)
            def _(p=p):
                e_copy(p, lax.rem(p - me + N_ROW, N_ROW)).start()

    def pair_rows(n):
        await_all(pair_in.at[n], y_recv.at[n])
        pair[n] = sp[n, side_y] + pair_in[n]
        for dz in range(1, N_PAIR):
            rs_copy(n, dz).start()

    def reduce_rows(n):
        await_all(rs_buf.at[n, pl.ds(1, N_PAIR - 1)], rs_recv.at[n])
        total = pair[n, at_z]
        for dz in range(1, N_PAIR):
            total = total + rs_buf[n, dz]
        own[n] = total
        for k, (p, at, sign) in enumerate(((0, 0, 1.0), (N_ROW - 1, width // N_ROW - 1, -1.0))):

            @pl.when(me == p)
            def _(k=k, at=at, sign=sign):
                await_all(fix_in.at[n, pl.ds(1, N_ROW - 1)], fix_recv.at[n])
                more = fix[n, k]
                for d in range(1, N_ROW):
                    more = more + fix_in[n, d]
                own[n, at : at + 1] = own[n, at : at + 1] + sign * more

        sall[n, side_y, at_z] = own[n]
        gather_first(n)

        @pl.when(lax.rem(me, 8) // 2 == n)
        def _():
            total = rim_send[me]
            await_all(rim_buf.at[pl.ds(1, N_ROW - 1)], e_recv)
            for d in range(1, N_ROW):
                total = total + rim_buf[d]
            rim_own[...] = total
            eall[me] = total
            for d in range(1, N_ROW):
                ea_copy(d).start()

    def velocity(n):
        await_gathered(n)
        mine = lax.rem(me, 8) // 2 == n
        for there, count in ((mine, 3), (jnp.logical_not(mine), 4)):

            @pl.when(there)
            def _(count=count):
                await_all(eall.at[pl.ds(0, count)], ea_recv.at[n])

        field = by_azimuth(sall, n)
        first, last = (jnp.concatenate([eall[p], eall[p + 1]], axis=1) for p in (2 * n, 8 + 2 * n))
        ahead = jnp.concatenate([field[1:], last], axis=0)
        behind = jnp.concatenate([first, field[:-1]], axis=0)
        now = (0.5 * geo_row(cells, n * tile, tile)) * (ahead - behind)
        lane = lax.broadcasted_iota(jnp.int32, (width, 128), 1)
        down = pltpu.roll(now, 1, axis=1)
        before = jnp.zeros((width, 128), F32) if n == 0 else carry_vel[...]
        carry_vel[...] = down[:, :128]
        down = jnp.concatenate([jnp.where(lane == 0, before, down[:, :128]), down[:, 128:]], axis=1)
        into = vel_last if n == stages - 1 else vel
        for k, x in enumerate(two_parts(down) + two_parts(now - down)):
            into[k * width : (k + 1) * width, :] = x

    def interpolate(n):
        def step(some, carry):
            for i in range(4 * (nodes // 256)):
                r, k = some * 4 + i // (nodes // 256), i % (nodes // 256)
                at = slice(k * 256, (k + 1) * 256)
                marks = one_hot(tile, n * tile - 1, low[pl.ds(r, 1), at])
                both = jnp.dot(vel[...], marks, preferred_element_type=F32)
                part = both[:width] + both[width : 2 * width]
                part = part + off[pl.ds(r, 1), at] * (both[2 * width : 3 * width] + both[3 * width :])
                pvt[r, :, at] = part if n == 0 else pvt[r, :, at] + part
            return carry

        lax.fori_loop(0, levels // 4, step, 0, unroll=2)

    def slopes(r):
        center = tv[r + 1]
        zero = jnp.zeros((1, width), F32)
        polar = jnp.concatenate([center[1:], zero], axis=0) - jnp.concatenate([zero, center[:-1]], axis=0)
        slope[r] = sines[...] * (tv[r + 2] - tv[r]) + cosines[...] * polar

    def finish():
        for side, there, comes in ((0, me > 0, me < N_ROW - 1), (1, me < N_ROW - 1, me > 0)):

            @pl.when(there)
            def _(side=side):
                await_all(tv.at[0], h_send.at[side])

            @pl.when(comes)
            def _(side=side):
                await_all(tv.at[0], h_recv.at[side])

    plan = iter(zip((0,) + HALO_PLAN, HALO_PLAN))
    for n in range(stages):
        sum_columns(n)
        send_inner(n)
        if n > 0:
            send_outer(n - 1)
        if n > 1:
            pair_rows(n - 2)
        halo_start(*next(plan))
    for copy in loads[5:]:
        copy.wait()
    for r in range(1, levels - 1):
        slopes(r)
    pair_rows(2)
    reduce_rows(0)
    send_outer(3)
    halo_start(*next(plan))
    pair_rows(3)
    halo_start(*next(plan))
    reduce_rows(1)
    halo_start(*next(plan))
    forward(0)
    reduce_rows(2)
    halo_start(*next(plan))
    reduce_rows(3)
    forward(2)
    forward(1)
    halo_start(*next(plan))
    velocity(0)
    forward(3)
    interpolate(0)
    velocity(1)
    interpolate(1)
    velocity(2)
    interpolate(2)
    finish()
    slopes(0)
    slopes(levels - 1)
    velocity(stages - 1)
    await_all(pair_in, y_send)
    await_all(rs_buf.at[:, pl.ds(1, N_PAIR - 1)], rs_send)
    for n in range(stages):
        await_sent(n)
    inner = jnp.logical_and(me > 0, me < N_ROW - 1)
    for there, count in ((inner, 8), (jnp.logical_not(inner), 4)):

        @pl.when(there)
        def _(count=count):
            await_all(fix_in.at[0, pl.ds(0, count)], fix_send)

    for sem in (e_send, ea_send):
        await_all(rim_buf.at[pl.ds(1, N_ROW - 1)], sem)


def advance_kernel(tv, pvt, vel, sall, slope, low, off, holder, stream, out_hbm, flow, drift, out, out_sem):
    levels, nodes, width = out.shape
    cells = holder.shape[1]
    stages, tile = sall.shape[0], sall.shape[4]
    me = lax.axis_index("row")

    def blend(r):
        for k in range(nodes // 256):
            at = slice(k * 256, (k + 1) * 256)
            marks = one_hot(tile, (stages - 1) * tile - 1, low[pl.ds(r, 1), at])
            both = jnp.dot(vel[...], marks, preferred_element_type=F32)
            part = pvt[r, :, at] + both[:width] + both[width : 2 * width]
            drift[lax.rem(r, 2), :, at] = part + off[pl.ds(r, 1), at] * (both[2 * width : 3 * width] + both[3 * width :])

    def update(r):
        out[r] = tv[r + 1] - drift[lax.rem(r, 2)].T * slope[r]
        pltpu.make_async_copy(out.at[r], out_hbm.at[r], out_sem.at[r]).start()

    def step(r, carry):
        update(r - 1)
        blend(r)
        return carry

    blend(0)
    lax.fori_loop(1, levels, step, 0, unroll=levels - 1)
    update(levels - 1)
    spots = own_slots(holder[...], me, stream.shape[0])
    held = jnp.zeros((2 * width, stream.shape[0]), F32)
    for n in range(stages):
        field = jnp.concatenate(two_parts(by_azimuth(sall, n)), axis=0)
        held = held + lax.dot_general(field, spots[:, n * tile : (n + 1) * tile], NT, preferred_element_type=F32)
    held = (held[:width] + held[width:]).T
    count = jnp.sum((holder[...] == me).astype(F32), axis=1, keepdims=True).astype(jnp.int32)
    slot = lax.broadcasted_iota(jnp.int32, held.shape, 0)
    flow[...] = jnp.where(slot < count, held, stream[...])
    for r in range(levels):
        pltpu.make_async_copy(out.at[r], out_hbm.at[r], out_sem.at[r]).wait()


VMEM = pl.BlockSpec(memory_space=pltpu.VMEM)
HBM = pl.BlockSpec(memory_space=pltpu.HBM)
DMA = pltpu.SemaphoreType.DMA


def per_device(heat, lower, offset, share, holder, stream):
    levels, nodes, width = heat.shape
    cells = holder.shape[0]
    slots = stream.shape[0]
    holder = holder.reshape(1, cells)
    angle = math.pi * (np.arange(nodes, dtype=np.float32) + np.float32(0.5)) / nodes
    sines = jnp.asarray(np.repeat((0.125 * np.sin(angle)).astype(np.float32)[:, None], width, axis=1))
    cosines = jnp.asarray(np.repeat((0.125 * np.cos(angle)).astype(np.float32)[:, None], width, axis=1))
    params = functools.partial(pltpu.CompilerParams, vmem_limit_bytes=40 << 20)

    rows = width // N_ROW
    stages = 4
    tile = cells // stages
    tv, pvt, vel, sall, slope = pl.pallas_call(
        fused_kernel,
        out_shape=(
            jax.ShapeDtypeStruct((levels + 2, nodes, width), F32),
            jax.ShapeDtypeStruct((levels, width, nodes), F32),
            jax.ShapeDtypeStruct((4 * width, tile), BF16),
            jax.ShapeDtypeStruct((stages, 2, N_PAIR, rows, tile), F32),
            jax.ShapeDtypeStruct((levels, nodes, width), F32),
        ),
        in_specs=[HBM] * 8,
        out_specs=(VMEM,) * 5,
        scratch_shapes=[
            pltpu.VMEM((nodes, width), F32),
            pltpu.VMEM((nodes, width), F32),
            pltpu.VMEM((levels, nodes), jnp.int32),
            pltpu.VMEM((levels, nodes), F32),
            pltpu.VMEM((levels, nodes), F32),
            pltpu.VMEM((1, cells), jnp.int32),
            pltpu.VMEM((slots, width), F32),
            pltpu.VMEM((width, cells), F32),
            pltpu.VMEM((levels, 4 * width, nodes), BF16),
            pltpu.VMEM((stages, 2, N_PAIR, rows, tile), F32),
            pltpu.VMEM((stages, N_PAIR, rows, tile), F32),
            pltpu.VMEM((stages, N_PAIR, rows, tile), F32),
            pltpu.VMEM((stages, 2, 2, tile), F32),
            pltpu.VMEM((stages, 2, 2, tile), F32),
            pltpu.VMEM((stages, 2, 1, tile), F32),
            pltpu.VMEM((stages, N_ROW, 1, tile), F32),
            pltpu.VMEM((N_ROW, 1, 128), F32),
            pltpu.VMEM((stages, N_PAIR, rows, tile), F32),
            pltpu.VMEM((N_ROW, 1, 128), F32),
            pltpu.VMEM((stages, rows, tile), F32),
            pltpu.VMEM((1, 128), F32),
            pltpu.VMEM((N_ROW, 1, 128), F32),
            pltpu.VMEM((width, 128), F32),
            pltpu.VMEM((width, 128), F32),
            pltpu.VMEM((4 * width, tile), BF16),
            DMA((levels,)), DMA((7,)),
            DMA, DMA((stages,)), DMA, DMA((stages,)),
            DMA, DMA((stages,)), DMA((stages,)), DMA((stages,)), DMA((stages,)), DMA((stages,)),
            DMA, DMA, DMA, DMA((stages,)),
            DMA((stages, 2)), DMA((stages, 2)), DMA((2,)), DMA((2,)),
        ],
        compiler_params=params(collective_id=0, has_side_effects=True),
        name="columns",
    )(*(pltpu.with_memory_space_constraint(x, pltpu.HBM) for x in (heat, lower, offset, share, holder, stream, sines, cosines)))

    return pl.pallas_call(
        advance_kernel,
        out_shape=(jax.ShapeDtypeStruct(heat.shape, F32), jax.ShapeDtypeStruct((slots, width), F32)),
        in_specs=[VMEM] * 9,
        out_specs=(HBM, VMEM),
        scratch_shapes=[pltpu.VMEM((2, width, nodes), F32), pltpu.VMEM((levels, nodes, width), F32), DMA((levels,))],
        compiler_params=params(),
        name="advance",
    )(tv, pvt, vel, sall, slope, lower, offset, holder, stream)


def solution(mesh):
    return jax.shard_map(
        per_device,
        mesh=mesh,
        in_specs=(P("row", None, "ma"), P("row", None), P("row", None), P("row", None), P(), P("row", "ma")),
        out_specs=(P("row", None, "ma"), P("row", "ma")),
        check_vma=False,
    )
```

```python
import functools
import math

import jax
import jax.numpy as jnp
import numpy as np
from jax import lax
from jax.experimental import pallas as pl
from jax.experimental.pallas import tpu as pltpu
from jax.sharding import PartitionSpec as P

MESH = pl.DeviceIdType.MESH
F32 = jnp.float32
BF16 = jnp.bfloat16
N_ROW = 16
N_PAIR = 8
N_MA = 16
HALO_PLAN = (2, 3, 3, 3, 5, 6, 7, 8, 9, 12)
Y_LAST = (0,)
NT = (((1,), (1,)), ((), ()))


def two_parts(x):
    hi = x.astype(BF16)
    return hi, (x - hi.astype(F32)).astype(BF16)


def one_hot(rows, first, index):
    at = lax.broadcasted_iota(jnp.int32, (rows, index.shape[1]), 0)
    return jnp.where(at == index - first, 1.0, 0.0).astype(BF16)


def geo_row(cells, first, count):
    c = (first + lax.broadcasted_iota(jnp.int32, (1, count), 1)).astype(F32)
    return 1.0 / (0.25 + (c + 0.5) / cells)


def by_azimuth(gathered, n):
    half, pairs, rows, tile = gathered.shape[1:]
    return jnp.stack([gathered[n, k] for k in range(half)], axis=1).reshape(half * pairs * rows, tile)


def own_slots(holder, me, slots):
    cells = holder.shape[1]
    start = jnp.sum((holder < me).astype(F32), axis=1, keepdims=True).astype(jnp.int32)
    c = lax.broadcasted_iota(jnp.int32, (1, cells), 1)
    return one_hot(slots, 0, jnp.where(holder == me, c - start, -1))


def fused_kernel(
    t_hbm, low_hbm, off_hbm, share_hbm, holder_hbm, stream_hbm, sin_hbm, cos_hbm,
    tv, pvt, vel_last, sall, slope,
    sines, cosines, low, off, share, holder, stream_in, stream, twt, sp, pair_in, pair, edge, rim, fix, fix_in, rim_send, rs_buf, rim_buf, own, rim_own, eall, carry_up, carry_vel, vel,
    t_sem, in_sem, y_send, y_recv, fix_send, fix_recv, rs_send, rs_recv, ag_send, ag_recv, agy_send, agy_recv, e_send, e_recv, ea_send, ea_recv, ma_send, ma_recv, h_send, h_recv,
):
    levels, width, nodes = pvt.shape
    cells = holder.shape[1]
    stages, tile = sp.shape[0], sp.shape[4]
    me = lax.axis_index("row")
    side_y, at_z = lax.rem(me, 2), me // 2
    partner = me + 1 - 2 * side_y
    ma = lax.axis_index("ma")
    right, left = lax.rem(ma + 1, N_MA), lax.rem(ma + N_MA - 1, N_MA)
    parts = HALO_PLAN[-1]
    piece = nodes // parts

    small = [(holder_hbm, holder), (stream_hbm, stream_in), (share_hbm, share), (off_hbm, off), (low_hbm, low), (sin_hbm, sines), (cos_hbm, cosines)]
    loads = [pltpu.make_async_copy(src, dst, in_sem.at[k]) for k, (src, dst) in enumerate(small)]
    heat_loads = [pltpu.make_async_copy(t_hbm.at[r], tv.at[r + 1], t_sem.at[r]) for r in range(levels)]
    for copy in loads + heat_loads:
        copy.start()
    barrier = pltpu.get_barrier_semaphore()
    for d in range(1, N_ROW):
        pl.semaphore_signal(barrier, inc=1, device_id={"row": lax.rem(me + d, N_ROW)}, device_id_type=MESH)
    for side in (left, right):
        pl.semaphore_signal(barrier, inc=1, device_id={"ma": side}, device_id_type=MESH)

    @pl.when(me == 0)
    def _():
        tv[0] = jnp.zeros((nodes, width), F32)

    @pl.when(me == N_ROW - 1)
    def _():
        tv[levels + 1] = jnp.zeros((nodes, width), F32)

    for copy in loads[:5]:
        copy.wait()
    spots = own_slots(holder[...], me, stream_in.shape[0])
    placed = jnp.dot(jnp.concatenate(two_parts(stream_in[...].T), axis=0), spots, preferred_element_type=F32)
    stream[...] = placed[:width] + placed[width:]

    def prepare(r):
        weights = share[r : r + 1, :]
        offset = off[r : r + 1, :]
        heat = tv[r + 1].T
        for k, weight in enumerate((weights * (1.0 - offset), weights * offset)):
            hi, lo = two_parts(heat * weight)
            twt[r, 2 * k * width : (2 * k + 1) * width, :] = hi
            twt[r, (2 * k + 1) * width : (2 * k + 2) * width, :] = lo


    def to_row(src, dst, send, recv, peer):
        return pltpu.make_async_remote_copy(src_ref=src, dst_ref=dst, send_sem=send, recv_sem=recv, device_id={"row": peer}, device_id_type=MESH)

    def await_all(like, sem):
        pltpu.make_async_copy(like, like, sem).wait()

    def halo(side, k):
        peer = jnp.maximum(me - 1, 0) if side == 0 else jnp.minimum(me + 1, N_ROW - 1)
        at = pl.ds(k * piece, piece)
        mine, theirs = (1, levels + 1) if side == 0 else (levels, 0)
        return to_row(tv.at[mine, at], tv.at[theirs, at], h_send.at[side], h_recv.at[side], peer)

    def halo_start(first, last):
        for side, there in ((0, me > 0), (1, me < N_ROW - 1)):

            @pl.when(there)
            def _(side=side):
                for k in range(first, last):
                    halo(side, k).start()

    def pieces(n):
        return (2 * n, 2 * n + 1, 8 + 2 * n, 8 + 2 * n + 1)

    def rim_copies(n):
        return [
            pltpu.make_async_remote_copy(src_ref=edge.at[n, k], dst_ref=rim.at[n, k], send_sem=ma_send.at[n, k], recv_sem=ma_recv.at[n, k], device_id={"ma": side}, device_id_type=MESH)
            for k, side in enumerate((left, right))
        ]

    def y_copy(n):
        return to_row(sp.at[n, 1 - side_y], pair_in.at[n], y_send, y_recv.at[n], partner)

    def rs_copy(n, dz):
        z = lax.rem(at_z + dz, N_PAIR)
        return to_row(pair.at[n, z], rs_buf.at[n, dz], rs_send, rs_recv.at[n], 2 * z + side_y)

    def fix_copy(n, k, p):
        d = lax.rem(p - me + N_ROW, N_ROW)
        return to_row(fix.at[n, k], fix_in.at[n, d], fix_send, fix_recv.at[n], p)

    def along_z(src, n, half):
        for dz in range(1, N_PAIR):
            peer = 2 * lax.rem(at_z + dz, N_PAIR) + side_y
            to_row(src, sall.at[n, half, at_z], ag_send.at[n], ag_recv.at[n], peer).start()

    def gather_first(n):
        if n not in Y_LAST:
            to_row(own.at[n], sall.at[n, side_y, at_z], agy_send.at[n], agy_recv.at[n], partner).start()
        along_z(own.at[n], n, side_y)

    def forward(n):
        if n in Y_LAST:
            await_all(rs_buf.at[n, pl.ds(1, N_PAIR - 1)], ag_recv.at[n])
            to_row(sall.at[n, side_y], sall.at[n, side_y], agy_send.at[n], agy_recv.at[n], partner).start()
        else:
            await_all(own.at[n], agy_recv.at[n])
            along_z(sall.at[n, 1 - side_y, at_z], n, 1 - side_y)

    def await_gathered(n):
        if n in Y_LAST:
            await_all(pair.at[n], agy_recv.at[n])
        else:
            await_all(rs_buf.at[pl.ds(0, 2), pl.ds(1, N_PAIR - 1)], ag_recv.at[n])

    def await_sent(n):
        if n in Y_LAST:
            await_all(rs_buf.at[n, pl.ds(1, N_PAIR - 1)], ag_send.at[n])
            await_all(pair.at[n], agy_send.at[n])
        else:
            await_all(rs_buf.at[pl.ds(0, 2), pl.ds(1, N_PAIR - 1)], ag_send.at[n])
            await_all(own.at[n], agy_send.at[n])

    def e_copy(p, d):
        return to_row(rim_send.at[p], rim_buf.at[d], e_send, e_recv, p)

    def ea_copy(d):
        return to_row(rim_own, eall.at[me], ea_send, ea_recv.at[lax.rem(me, 8) // 2], lax.rem(me + d, N_ROW))

    def sum_columns(n):
        sums = [jnp.zeros((4 * width, tile), F32)] * 2
        for r in range(levels):
            if n == 0:
                if r % 4 == 0:
                    for copy in heat_loads[r : r + 4]:
                        copy.wait()
                if r == 4:
                    pl.semaphore_wait(barrier, N_ROW + 1)
                    halo_start(*next(plan))
                prepare(r)
            marks = one_hot(tile, n * tile, low[r : r + 1, :])
            sums[r % 2] = sums[r % 2] + lax.dot_general(twt[r], marks, NT, preferred_element_type=F32)
        half = 2 * width
        here, following = (0.25 * geo_row(cells, n * tile + k, tile) for k in range(2))
        lower = here * sums[0][:half] + here * sums[1][:half]
        lower = lower[:width] + lower[width:]
        upper = following * sums[0][half:] + following * sums[1][half:]
        upper = pltpu.roll(upper[:width] + upper[width:], 1, axis=1)
        lane = lax.broadcasted_iota(jnp.int32, (width, 128), 1)
        before = jnp.zeros((width, 128), F32) if n == 0 else carry_up[...]
        carry_up[...] = upper[:, :128]
        upper = jnp.concatenate([jnp.where(lane == 0, before, upper[:, :128]), upper[:, 128:]], axis=1)
        zint = lower + upper
        zero = jnp.zeros((1, tile), F32)
        ahead = jnp.concatenate([zint[1:], zero], axis=0)
        behind = jnp.concatenate([zero, zint[:-1]], axis=0)
        partial = stream[:, n * tile : (n + 1) * tile] - (ahead - behind)
        chunks = partial.reshape(N_PAIR, 2, width // N_ROW, tile)
        for k in range(2):
            sp[n, k] = chunks[:, k]
        edge[n, 0] = jnp.concatenate([zint[:1], partial[:1]], axis=0)
        edge[n, 1] = jnp.concatenate([zint[-1:], partial[-1:]], axis=0)

    def send_inner(n):
        for copy in rim_copies(n):
            copy.start()
        y_copy(n).start()

    def send_outer(n):
        for copy in rim_copies(n):
            copy.wait()
        fix[n, 0] = rim[n, 1, 0:1]
        fix[n, 1] = rim[n, 0, 0:1]
        outer = (rim[n, 1, 1:2] - edge[n, 0, 0:1], rim[n, 0, 1:2] + edge[n, 1, 0:1])
        for i, p in enumerate(pieces(n)):
            rim_send[p] = outer[i // 2][:, (i % 2) * 128 : (i % 2 + 1) * 128]
        for k, p in enumerate((0, N_ROW - 1)):

            @pl.when(me != p)
            def _(k=k, p=p):
                fix_copy(n, k, p).start()

        for p in pieces(n):

            @pl.when(me != p)
            def _(p=p):
                e_copy(p, lax.rem(p - me + N_ROW, N_ROW)).start()

    def pair_rows(n):
        await_all(pair_in.at[n], y_recv.at[n])
        pair[n] = sp[n, side_y] + pair_in[n]
        for dz in range(1, N_PAIR):
            rs_copy(n, dz).start()

    def reduce_rows(n):
        await_all(rs_buf.at[n, pl.ds(1, N_PAIR - 1)], rs_recv.at[n])
        total = pair[n, at_z]
        for dz in range(1, N_PAIR):
            total = total + rs_buf[n, dz]
        own[n] = total
        for k, (p, at, sign) in enumerate(((0, 0, 1.0), (N_ROW - 1, width // N_ROW - 1, -1.0))):

            @pl.when(me == p)
            def _(k=k, at=at, sign=sign):
                await_all(fix_in.at[n, pl.ds(1, N_ROW - 1)], fix_recv.at[n])
                more = fix[n, k]
                for d in range(1, N_ROW):
                    more = more + fix_in[n, d]
                own[n, at : at + 1] = own[n, at : at + 1] + sign * more

        sall[n, side_y, at_z] = own[n]
        gather_first(n)

        @pl.when(lax.rem(me, 8) // 2 == n)
        def _():
            total = rim_send[me]
            await_all(rim_buf.at[pl.ds(1, N_ROW - 1)], e_recv)
            for d in range(1, N_ROW):
                total = total + rim_buf[d]
            rim_own[...] = total
            eall[me] = total
            for d in range(1, N_ROW):
                ea_copy(d).start()

    def velocity(n):
        await_gathered(n)
        mine = lax.rem(me, 8) // 2 == n
        for there, count in ((mine, 3), (jnp.logical_not(mine), 4)):

            @pl.when(there)
            def _(count=count):
                await_all(eall.at[pl.ds(0, count)], ea_recv.at[n])

        field = by_azimuth(sall, n)
        first, last = (jnp.concatenate([eall[p], eall[p + 1]], axis=1) for p in (2 * n, 8 + 2 * n))
        ahead = jnp.concatenate([field[1:], last], axis=0)
        behind = jnp.concatenate([first, field[:-1]], axis=0)
        now = (0.5 * geo_row(cells, n * tile, tile)) * (ahead - behind)
        lane = lax.broadcasted_iota(jnp.int32, (width, 128), 1)
        down = pltpu.roll(now, 1, axis=1)
        before = jnp.zeros((width, 128), F32) if n == 0 else carry_vel[...]
        carry_vel[...] = down[:, :128]
        down = jnp.concatenate([jnp.where(lane == 0, before, down[:, :128]), down[:, 128:]], axis=1)
        into = vel_last if n == stages - 1 else vel
        for k, x in enumerate(two_parts(down) + two_parts(now - down)):
            into[k * width : (k + 1) * width, :] = x

    def interpolate(n):
        def step(some, carry):
            for i in range(4 * (nodes // 256)):
                r, k = some * 4 + i // (nodes // 256), i % (nodes // 256)
                at = slice(k * 256, (k + 1) * 256)
                marks = one_hot(tile, n * tile - 1, low[pl.ds(r, 1), at])
                both = jnp.dot(vel[...], marks, preferred_element_type=F32)
                part = both[:width] + both[width : 2 * width]
                part = part + off[pl.ds(r, 1), at] * (both[2 * width : 3 * width] + both[3 * width :])
                pvt[r, :, at] = part if n == 0 else pvt[r, :, at] + part
            return carry

        lax.fori_loop(0, levels // 4, step, 0, unroll=2)

    def slopes(r):
        center = tv[r + 1]
        zero = jnp.zeros((1, width), F32)
        polar = jnp.concatenate([center[1:], zero], axis=0) - jnp.concatenate([zero, center[:-1]], axis=0)
        slope[r] = sines[...] * (tv[r + 2] - tv[r]) + cosines[...] * polar

    def finish():
        for side, there, comes in ((0, me > 0, me < N_ROW - 1), (1, me < N_ROW - 1, me > 0)):

            @pl.when(there)
            def _(side=side):
                await_all(tv.at[0], h_send.at[side])

            @pl.when(comes)
            def _(side=side):
                await_all(tv.at[0], h_recv.at[side])

    plan = iter(zip((0,) + HALO_PLAN, HALO_PLAN))
    for n in range(stages):
        sum_columns(n)
        send_inner(n)
        if n > 0:
            send_outer(n - 1)
        if n > 1:
            pair_rows(n - 2)
        halo_start(*next(plan))
    for copy in loads[5:]:
        copy.wait()
    for r in range(1, levels - 1):
        slopes(r)
    pair_rows(2)
    reduce_rows(0)
    send_outer(3)
    halo_start(*next(plan))
    pair_rows(3)
    halo_start(*next(plan))
    reduce_rows(1)
    halo_start(*next(plan))
    forward(1)
    forward(0)
    reduce_rows(2)
    halo_start(*next(plan))
    reduce_rows(3)
    forward(2)
    halo_start(*next(plan))
    velocity(0)
    forward(3)
    interpolate(0)
    velocity(1)
    interpolate(1)
    velocity(2)
    interpolate(2)
    finish()
    slopes(0)
    slopes(levels - 1)
    velocity(stages - 1)
    await_all(pair_in, y_send)
    await_all(rs_buf.at[:, pl.ds(1, N_PAIR - 1)], rs_send)
    for n in range(stages):
        await_sent(n)
    inner = jnp.logical_and(me > 0, me < N_ROW - 1)
    for there, count in ((inner, 8), (jnp.logical_not(inner), 4)):

        @pl.when(there)
        def _(count=count):
            await_all(fix_in.at[0, pl.ds(0, count)], fix_send)

    for sem in (e_send, ea_send):
        await_all(rim_buf.at[pl.ds(1, N_ROW - 1)], sem)


def advance_kernel(tv, pvt, vel, sall, slope, low, off, holder, stream, out_hbm, flow, drift, out, out_sem):
    levels, nodes, width = out.shape
    cells = holder.shape[1]
    stages, tile = sall.shape[0], sall.shape[4]
    me = lax.axis_index("row")

    def blend(r):
        for k in range(nodes // 256):
            at = slice(k * 256, (k + 1) * 256)
            marks = one_hot(tile, (stages - 1) * tile - 1, low[pl.ds(r, 1), at])
            both = jnp.dot(vel[...], marks, preferred_element_type=F32)
            part = pvt[r, :, at] + both[:width] + both[width : 2 * width]
            drift[lax.rem(r, 2), :, at] = part + off[pl.ds(r, 1), at] * (both[2 * width : 3 * width] + both[3 * width :])

    def update(r):
        out[r] = tv[r + 1] - drift[lax.rem(r, 2)].T * slope[r]
        pltpu.make_async_copy(out.at[r], out_hbm.at[r], out_sem.at[r]).start()

    def step(r, carry):
        update(r - 1)
        blend(r)
        return carry

    blend(0)
    lax.fori_loop(1, levels, step, 0, unroll=levels - 1)
    update(levels - 1)
    spots = own_slots(holder[...], me, stream.shape[0])
    held = jnp.zeros((2 * width, stream.shape[0]), F32)
    for n in range(stages):
        field = jnp.concatenate(two_parts(by_azimuth(sall, n)), axis=0)
        held = held + lax.dot_general(field, spots[:, n * tile : (n + 1) * tile], NT, preferred_element_type=F32)
    held = (held[:width] + held[width:]).T
    count = jnp.sum((holder[...] == me).astype(F32), axis=1, keepdims=True).astype(jnp.int32)
    slot = lax.broadcasted_iota(jnp.int32, held.shape, 0)
    flow[...] = jnp.where(slot < count, held, stream[...])
    for r in range(levels):
        pltpu.make_async_copy(out.at[r], out_hbm.at[r], out_sem.at[r]).wait()


VMEM = pl.BlockSpec(memory_space=pltpu.VMEM)
HBM = pl.BlockSpec(memory_space=pltpu.HBM)
DMA = pltpu.SemaphoreType.DMA


def per_device(heat, lower, offset, share, holder, stream):
    levels, nodes, width = heat.shape
    cells = holder.shape[0]
    slots = stream.shape[0]
    holder = holder.reshape(1, cells)
    angle = math.pi * (np.arange(nodes, dtype=np.float32) + np.float32(0.5)) / nodes
    sines = jnp.asarray(np.repeat((0.125 * np.sin(angle)).astype(np.float32)[:, None], width, axis=1))
    cosines = jnp.asarray(np.repeat((0.125 * np.cos(angle)).astype(np.float32)[:, None], width, axis=1))
    params = functools.partial(pltpu.CompilerParams, vmem_limit_bytes=40 << 20)

    rows = width // N_ROW
    stages = 4
    tile = cells // stages
    tv, pvt, vel, sall, slope = pl.pallas_call(
        fused_kernel,
        out_shape=(
            jax.ShapeDtypeStruct((levels + 2, nodes, width), F32),
            jax.ShapeDtypeStruct((levels, width, nodes), F32),
            jax.ShapeDtypeStruct((4 * width, tile), BF16),
            jax.ShapeDtypeStruct((stages, 2, N_PAIR, rows, tile), F32),
            jax.ShapeDtypeStruct((levels, nodes, width), F32),
        ),
        in_specs=[HBM] * 8,
        out_specs=(VMEM,) * 5,
        scratch_shapes=[
            pltpu.VMEM((nodes, width), F32),
            pltpu.VMEM((nodes, width), F32),
            pltpu.VMEM((levels, nodes), jnp.int32),
            pltpu.VMEM((levels, nodes), F32),
            pltpu.VMEM((levels, nodes), F32),
            pltpu.VMEM((1, cells), jnp.int32),
            pltpu.VMEM((slots, width), F32),
            pltpu.VMEM((width, cells), F32),
            pltpu.VMEM((levels, 4 * width, nodes), BF16),
            pltpu.VMEM((stages, 2, N_PAIR, rows, tile), F32),
            pltpu.VMEM((stages, N_PAIR, rows, tile), F32),
            pltpu.VMEM((stages, N_PAIR, rows, tile), F32),
            pltpu.VMEM((stages, 2, 2, tile), F32),
            pltpu.VMEM((stages, 2, 2, tile), F32),
            pltpu.VMEM((stages, 2, 1, tile), F32),
            pltpu.VMEM((stages, N_ROW, 1, tile), F32),
            pltpu.VMEM((N_ROW, 1, 128), F32),
            pltpu.VMEM((stages, N_PAIR, rows, tile), F32),
            pltpu.VMEM((N_ROW, 1, 128), F32),
            pltpu.VMEM((stages, rows, tile), F32),
            pltpu.VMEM((1, 128), F32),
            pltpu.VMEM((N_ROW, 1, 128), F32),
            pltpu.VMEM((width, 128), F32),
            pltpu.VMEM((width, 128), F32),
            pltpu.VMEM((4 * width, tile), BF16),
            DMA((levels,)), DMA((7,)),
            DMA, DMA((stages,)), DMA, DMA((stages,)),
            DMA, DMA((stages,)), DMA((stages,)), DMA((stages,)), DMA((stages,)), DMA((stages,)),
            DMA, DMA, DMA, DMA((stages,)),
            DMA((stages, 2)), DMA((stages, 2)), DMA((2,)), DMA((2,)),
        ],
        compiler_params=params(collective_id=0, has_side_effects=True),
        name="columns",
    )(*(pltpu.with_memory_space_constraint(x, pltpu.HBM) for x in (heat, lower, offset, share, holder, stream, sines, cosines)))

    return pl.pallas_call(
        advance_kernel,
        out_shape=(jax.ShapeDtypeStruct(heat.shape, F32), jax.ShapeDtypeStruct((slots, width), F32)),
        in_specs=[VMEM] * 9,
        out_specs=(HBM, VMEM),
        scratch_shapes=[pltpu.VMEM((2, width, nodes), F32), pltpu.VMEM((levels, nodes, width), F32), DMA((levels,))],
        compiler_params=params(),
        name="advance",
    )(tv, pvt, vel, sall, slope, lower, offset, holder, stream)


def solution(mesh):
    return jax.shard_map(
        per_device,
        mesh=mesh,
        in_specs=(P("row", None, "ma"), P("row", None), P("row", None), P("row", None), P(), P("row", "ma")),
        out_specs=(P("row", None, "ma"), P("row", "ma")),
        check_vma=False,
    )
```
